32 devices in a mesh: dp: 16 (over z, x, core), seq: 2 (over y).
Axes of the slice: x: 2, y: 2, z: 4, core: 2. Of those that a mesh axis runs over, the one named last changes fastest.
Arguments:
- frames: bfloat16 [16, 1024, 512], P('dp', 'seq'), may hold values from -6 to 6
- cotangent: bfloat16 [16, 1024, 512], P('dp', 'seq'), may hold values from -6 to 6
- weight_in: bfloat16 [2, 512, 2176], replicated, may hold values from -0.25 to 0.25
- qk_scales: float32 [2, 2, 128], replicated, may hold values from 0.5 to 1.5
- weight_out: bfloat16 [2, 1024, 512], replicated, may hold values from -0.1875 to 0.1875
- gains: float32 [2, 512], replicated, may hold values from 0.5 to 1.5
Outputs:
- output: bfloat16 [16, 1024, 512], P('dp', 'seq')
- grad_frames: bfloat16 [16, 1024, 512], P('dp', 'seq')
- grad_in: float32 [2, 512, 2176], P(None, 'dp')
- grad_out: float32 [2, 1024, 512], P(None, 'dp')
- grad_gains: float32 [2, 512], replicated
- grad_scales: float32 [2, 2, 128], replicated
The draws below stay inside these ranges and needn't reach their ends.
All inputs are finite; a program needn't handle non-finite values.
Results may differ from the reference program's by a relative error of at most 0.028.
Values may be sent and summed in bfloat16 or wider, within the bound.
A program may use at most 192 MiB of HBM per device.

```python
from functools import partial
import jax
import jax.numpy as jnp
from jax import lax

D = 512
E = 1024
S = 128
BLOCK = 256
NCH = 4
SEQLEN = 1024
BATCH = 16


def steps_of(own_key, extent, cuts, low, top_value):
    factor_of, own = 1.0, jax.random.fold_in(own_key, 6)
    for axis_at, shards_of in cuts:
        draws = jnp.exp(jax.random.uniform(jax.random.fold_in(own, axis_at), (shards_of,), jnp.float32, low / len(cuts), top_value / len(cuts)))
        factor_of = factor_of * jnp.repeat(draws, extent[axis_at] // shards_of).reshape([-1 if axis == axis_at else 1 for axis in range(len(extent))])
    return factor_of


def bell_draw(key, extent, scale, limit, cuts=(), held_as=jnp.bfloat16):
    entries = scale * jax.random.normal(key, extent, jnp.float32)
    if cuts:
        entries = entries * steps_of(key, extent, cuts, -0.22, 0.18)
    return jnp.clip(entries, -limit, limit).astype(held_as)


def setup_inputs(seed: int = 0) -> dict:
    key_list = jax.random.split(jax.random.key(seed), 7)
    frames = bell_draw(key_list[0], (BATCH, SEQLEN, D), 1.0, 6.0, ((0, 16), (1, 2)))
    cotangent = bell_draw(key_list[1], (BATCH, SEQLEN, D), 1.0, 6.0, ((0, 16), (1, 2)))
    weight_in = bell_draw(key_list[2], (2, D, 2 * E + S), D ** -0.5, 0.25)
    qk_scales = jnp.clip(1.0 + 0.1 * jax.random.normal(key_list[3], (2, 2, S), jnp.float32), 0.5, 1.5)
    weight_out = bell_draw(key_list[4], (2, E, D), E ** -0.5, 0.1875)
    gains = jnp.clip(1.0 + 0.1 * jax.random.normal(key_list[5], (2, D), jnp.float32), 0.5, 1.5)
    return dict(frames=frames, cotangent=cotangent, weight_in=weight_in, qk_scales=qk_scales, weight_out=weight_out, gains=gains)


EPSILON = 1e-06

def normed(values, gain_row):
    scaling = lax.rsqrt(lax.optimization_barrier(jnp.mean(values * values, axis=-1, keepdims=True)) + EPSILON)
    return values * scaling * gain_row

def mixer(projected, scale_pair, attend_axis):
    width = (projected.shape[-1] - scale_pair.shape[-1]) // 2
    active = jax.nn.silu(projected)
    gate_part = active[..., :width]
    value_part = active[..., width:2 * width].astype(jnp.bfloat16)
    shared = active[..., 2 * width:]
    query = (shared * scale_pair[0]).astype(jnp.bfloat16)
    keyed = (shared * scale_pair[1]).astype(jnp.bfloat16)
    length = projected.shape[attend_axis]
    if attend_axis == 1:
        score_form = 'gls,gms->glm'
        mix_form = 'glm,gme->gle'
    else:
        score_form = 'lgs,mgs->glm'
        mix_form = 'glm,mge->lge'
    scores = jnp.einsum(score_form, query.astype(jnp.float32), keyed.astype(jnp.float32))
    scores = scores * scale_pair.shape[-1] ** (-0.5)
    weights = (jnp.square(jax.nn.relu(scores)) / length).astype(jnp.bfloat16)
    mixed = jnp.einsum(mix_form, weights.astype(jnp.float32), value_part.astype(jnp.float32))
    return (gate_part * mixed).astype(jnp.bfloat16)

def rows_product(left, right):
    left_rows = left.reshape(-1, left.shape[-1])
    right_rows = right.reshape(-1, right.shape[-1])
    return lax.dot_general(left_rows, right_rows, (((0,), (0,)), ((), ())), preferred_element_type=jnp.float32)

def against(values, weight):
    return lax.dot_general(values, weight, (((values.ndim - 1,), (1,)), ((), ())), preferred_element_type=jnp.float32)

def unit_forward(inputs_now, weight_in, scale_pair, weight_out, gain_row, attend_axis):
    hidden = normed(inputs_now.astype(jnp.float32), gain_row).astype(jnp.bfloat16)
    projected = jnp.dot(hidden, weight_in, preferred_element_type=jnp.float32)
    gated = mixer(projected, scale_pair, attend_axis)
    result = (inputs_now.astype(jnp.float32) + jnp.dot(gated, weight_out, preferred_element_type=jnp.float32)).astype(jnp.bfloat16)
    return (result, (hidden, projected, gated))

def unit_backward(inputs_now, upstream, weight_in, scale_pair, weight_out, gain_row, saved, attend_axis):
    hidden, projected, gated = saved
    grad_out = rows_product(gated, upstream)
    grad_gated = against(upstream, weight_out).astype(jnp.bfloat16)
    pulled = jax.vjp(partial(mixer, attend_axis=attend_axis), projected, scale_pair)[1]
    grad_proj, grad_scale = pulled(grad_gated)
    grad_proj = grad_proj.astype(jnp.bfloat16)
    grad_in = rows_product(hidden, grad_proj)
    grad_hidden = against(grad_proj, weight_in)
    norm_pull = jax.vjp(normed, inputs_now.astype(jnp.float32), gain_row)[1]
    grad_inputs, grad_gain = norm_pull(grad_hidden)
    grad_inputs = (upstream.astype(jnp.float32) + grad_inputs).astype(jnp.bfloat16)
    return (grad_inputs, grad_in, grad_out, grad_gain, grad_scale)

def reference(frames, cotangent, weight_in, qk_scales, weight_out, gains):
    scaling = (BATCH * SEQLEN) ** (-0.5)

    def one_sequence(carry, pair):
        seq_frames, seq_cot = pair
        blocked = seq_frames.reshape(NCH, BLOCK, D)
        upstream = seq_cot.reshape(NCH, BLOCK, D)
        first, saved_first = unit_forward(blocked, weight_in[0], qk_scales[0], weight_out[0], gains[0], 1)
        second, saved_second = unit_forward(first, weight_in[1], qk_scales[1], weight_out[1], gains[1], 0)
        back_first, in_late, out_late, gain_late, scale_late = unit_backward(first, upstream, weight_in[1], qk_scales[1], weight_out[1], gains[1], saved_second, 0)
        back_frames, in_early, out_early, gain_early, scale_early = unit_backward(blocked, back_first, weight_in[0], qk_scales[0], weight_out[0], gains[0], saved_first, 1)
        carry = (carry[0] + jnp.stack([in_early, in_late]), carry[1] + jnp.stack([out_early, out_late]), carry[2] + jnp.stack([gain_early, gain_late]), carry[3] + jnp.stack([scale_early, scale_late]))
        return (carry, (second.reshape(SEQLEN, D), back_frames.reshape(SEQLEN, D)))
    start = (jnp.zeros((2, D, 2 * E + S), jnp.float32), jnp.zeros((2, E, D), jnp.float32), jnp.zeros((2, D), jnp.float32), jnp.zeros((2, 2, S), jnp.float32))
    totals, outs_pair = lax.scan(one_sequence, start, (frames, cotangent))
    return (outs_pair[0], outs_pair[1], totals[0] * scaling, totals[1] * scaling, totals[2] * scaling, totals[3] * scaling)
```

```python
from functools import partial
from functools import partial as partial_of

import jax
import jax.numpy as jnp
from jax import lax
from jax.experimental import pallas as pl
from jax.experimental.pallas import tpu as pltpu
from jax.sharding import PartitionSpec as P

BLOCK = 256


EPSILON = 1e-06


def normed(values, gain_row):
    scaling = lax.rsqrt(jnp.mean(values * values, axis=-1, keepdims=True) + EPSILON)
    return values * scaling * gain_row


def mixer(projected, scale_pair, attend_axis):
    width = (projected.shape[-1] - scale_pair.shape[-1]) // 2
    active = jax.nn.silu(projected)
    gate_part = active[..., :width]
    value_part = active[..., width : 2 * width].astype(jnp.bfloat16)
    shared = active[..., 2 * width :]
    query = (shared * scale_pair[0]).astype(jnp.bfloat16)
    keyed = (shared * scale_pair[1]).astype(jnp.bfloat16)
    length = projected.shape[attend_axis]
    if attend_axis == 1:
        score_form = "gls,gms->glm"
        mix_form = "glm,gme->gle"
    else:
        score_form = "lgs,mgs->glm"
        mix_form = "glm,mge->lge"
    scores = jnp.einsum(score_form, query, keyed, preferred_element_type=jnp.float32)
    scores = scores * scale_pair.shape[-1] ** (-0.5)
    weights = (jnp.square(jax.nn.relu(scores)) / length).astype(jnp.bfloat16)
    mixed = jnp.einsum(mix_form, weights, value_part, preferred_element_type=jnp.float32)
    return (gate_part * mixed).astype(jnp.bfloat16)


def rows_product(left, right):
    left_rows = left.reshape(-1, left.shape[-1])
    right_rows = right.reshape(-1, right.shape[-1])
    return lax.dot_general(
        left_rows, right_rows, (((0,), (0,)), ((), ())), preferred_element_type=jnp.float32
    )


def against(values, weight):
    return lax.dot_general(
        values, weight, (((values.ndim - 1,), (1,)), ((), ())), preferred_element_type=jnp.float32
    )


def unit_forward(inputs_now, weight_in, scale_pair, weight_out, gain_row, attend_axis):
    hidden = normed(inputs_now.astype(jnp.float32), gain_row).astype(jnp.bfloat16)
    projected = jnp.dot(hidden, weight_in, preferred_element_type=jnp.float32)
    gated = mixer(projected, scale_pair, attend_axis)
    result = (
        inputs_now.astype(jnp.float32)
        + jnp.dot(gated, weight_out, preferred_element_type=jnp.float32)
    ).astype(jnp.bfloat16)
    return (result, (hidden, projected, gated))


def unit_backward(
    inputs_now, upstream, weight_in, scale_pair, weight_out, gain_row, saved, attend_axis
):
    hidden, projected, gated = saved
    grad_out = rows_product(gated, upstream)
    grad_gated = against(upstream, weight_out).astype(jnp.bfloat16)
    pulled = jax.vjp(partial(mixer, attend_axis=attend_axis), projected, scale_pair)[1]
    grad_proj, grad_scale = pulled(grad_gated)
    grad_proj = grad_proj.astype(jnp.bfloat16)
    grad_in = rows_product(hidden, grad_proj)
    grad_hidden = against(grad_proj, weight_in)
    norm_pull = jax.vjp(normed, inputs_now.astype(jnp.float32), gain_row)[1]
    grad_inputs, grad_gain = norm_pull(grad_hidden)
    grad_inputs = (upstream.astype(jnp.float32) + grad_inputs).astype(jnp.bfloat16)
    return (grad_inputs, grad_in, grad_out, grad_gain, grad_scale)


def bit_of(axis, bit):
    return lax.rem(lax.axis_index(axis) // (1 << bit), 2)


def axis_bits(axis):
    return [(axis, bit) for bit in range(lax.axis_size(axis).bit_length() - 1)]


def partner(axis, bit):
    spot = {name: lax.axis_index(name) for name in ("dp", "seq")}
    spot[axis] = spot[axis] + (1 << bit) * (1 - 2 * bit_of(axis, bit))
    return (spot["dp"], spot["seq"])


def halving_order(turn):
    dp_bits, seq_bits = axis_bits("dp"), axis_bits("seq")
    rest = dp_bits[1:2] + seq_bits + dp_bits[2:-1]
    turn = turn % max(len(rest), 1)
    return dp_bits[:1] + rest[turn:] + rest[:turn] + dp_bits[2:][-1:]


def place_of(known, leading):
    return tuple(known.get(bit, slice(None)) for bit in leading)


SLOTS = ((0, 1), (1, 1), (1, 0), (0, 0))


class Sums:
    def __init__(self, plan, given, buffers):
        self.plan, self.given = plan, given
        self.small_held, self.small_got, self.sends, self.recvs = buffers[:4]
        buffers = buffers[4:]
        self.dp_bits, self.seq_bits = axis_bits("dp"), axis_bits("seq")
        self.leading = self.dp_bits[::-1] + self.seq_bits[::-1]
        self.steps = len(self.leading)
        total = len(plan)
        self.accs, self.gathers = buffers[:total], buffers[total : 2 * total]
        self.landings = [
            buffers[2 * total + self.steps * i : 2 * total + self.steps * (i + 1)]
            for i in range(total)
        ]
        self.mine = {bit: bit_of(*bit) for bit in self.leading}
        self.where = {bit: partner(*bit) for bit in self.leading}
        self.orders = [halving_order(turn) for _, _, _, turn in plan]
        self.flying = [None] * total
        self.known = [{} for _ in plan]
        self.at_step = [0] * total
        self.started = []
        self.small_step = 0

    def greet(self):
        barrier = pltpu.get_barrier_semaphore()
        for bit in self.leading:
            pl.semaphore_signal(
                barrier, inc=1, device_id=self.where[bit], device_id_type=pl.DeviceIdType.MESH
            )
        pl.semaphore_wait(barrier, self.steps)

    def copy(self, source, target, send_sem, recv_sem, bit):
        made = pltpu.make_async_remote_copy(
            src_ref=source,
            dst_ref=target,
            send_sem=send_sem,
            recv_sem=recv_sem,
            device_id=self.where[bit],
            device_id_type=pl.DeviceIdType.MESH,
        )
        made.start()
        self.started.append(made)
        return made

    def send(self, source, target, row, column, bit):
        return self.copy(
            source, target, self.sends.at[row, column], self.recvs.at[row, column], bit
        )

    def launch(self, index, step=0):
        array, low, high, _ = self.plan[index]
        order = self.orders[index]
        bit = order[step]
        if step == 0:
            place = place_of({bit: 1 - self.mine[bit]}, self.leading)
            source = self.given[array].at[place + (slice(None), slice(low, high))]
        else:
            left = [other for other in self.leading if other != order[0]]
            place = place_of({**self.known[index], bit: 1 - self.mine[bit]}, left)
            source = self.accs[index].at[place]
        self.flying[index] = self.send(source, self.landings[index][step], index, step, bit)

    def advance(self, index):
        step = self.at_step[index]
        if step >= self.steps or self.flying[index] is None:
            return
        array, low, high, _ = self.plan[index]
        order = self.orders[index]
        bit = order[step]
        self.flying[index].wait_recv()
        landed = self.landings[index][step]
        left = [other for other in self.leading if other != order[0]]
        acc = self.accs[index]
        if step == 0:
            place = place_of({bit: self.mine[bit]}, self.leading)
            acc[...] = self.given[array][place + (slice(None), slice(low, high))] + landed[...]
        else:
            self.known[index][bit] = self.mine[bit]
            place = place_of(self.known[index], left)
            acc[place] = acc[place] + landed[...]
        self.at_step[index] = step + 1
        if step + 1 < self.steps:
            self.launch(index, step + 1)
        else:
            spot = place_of(self.mine, self.seq_bits)
            self.gathers[index][spot] = acc[place_of(self.mine, left)]
            if self.seq_bits:
                held = self.gathers[index].at[spot]
                self.flying[index] = self.send(held, held, index, self.steps, self.seq_bits[0])

    def of_arrays(self, wanted):
        return [index for index, (array, _, _, _) in enumerate(self.plan) if array in wanted]

    def launch_all(self, *wanted):
        for index in self.of_arrays(wanted):
            self.launch(index)

    def advance_all(self, *wanted):
        for index in self.of_arrays(wanted):
            self.advance(index)

    def small_send(self):
        step = self.small_step
        self.small_copy = self.send(
            self.small_held.at[step],
            self.small_got.at[step],
            len(self.plan),
            step,
            self.leading[step],
        )

    def small_advance(self):
        step = self.small_step
        if step >= self.steps:
            return
        self.small_copy.wait_recv()
        self.small_held[step + 1] = self.small_held[step] + self.small_got[step]
        self.small_step = step + 1
        if step + 1 < self.steps:
            self.small_send()

    def finish(self, results, small_out, scaling, *order):
        while min(self.at_step) < self.steps:
            for wanted in order:
                self.advance_all(*wanted)
            self.small_advance()
        while self.small_step < self.steps:
            self.small_advance()
        small_out[...] = self.small_held[self.steps] * scaling
        total = len(self.plan)
        for turn in range(1, len(self.seq_bits)):
            for index in range(total):
                self.flying[index].wait_recv()
                have = {bit: self.mine[bit] for bit in self.seq_bits[turn:]}
                spot = self.gathers[index].at[place_of(have, self.seq_bits)]
                self.flying[index] = self.send(
                    spot, spot, index, self.steps + turn, self.seq_bits[turn]
                )
        for index in range(total):
            array, low, high, _ = self.plan[index]
            if self.seq_bits:
                self.flying[index].wait_recv()
            for part in range(1 << len(self.seq_bits)):
                spot = tuple((part >> bit) % 2 for _, bit in self.seq_bits)
                place, unit = SLOTS[array]
                results[place][unit, part, :, low:high] = (
                    self.gathers[index][spot].astype(jnp.float32) * scaling
                )
        for made in self.started:
            made.wait_send()


def sums_scratch(cuts, wide, lines):
    dp_bits, seq_bits = axis_bits("dp"), axis_bits("seq")
    steps = len(dp_bits) + len(seq_bits)
    accs, gathers, landings = [], [], []
    for array, low, high, _ in cuts:
        tail = (wide[array][-2], high - low)
        accs.append(pltpu.VMEM((2,) * (steps - 1) + tail, jnp.bfloat16))
        gathers.append(pltpu.VMEM((2,) * len(seq_bits) + tail, jnp.bfloat16))
        landings += [
            pltpu.VMEM((2,) * (steps - 1 - step) + tail, jnp.bfloat16) for step in range(steps)
        ]
    sems = pltpu.SemaphoreType.DMA((len(cuts) + 1, steps + len(seq_bits)))
    return [
        pltpu.VMEM((steps + 1,) + lines, jnp.float32),
        pltpu.VMEM((steps,) + lines, jnp.float32),
        sems,
        sems,
    ] + accs + gathers + landings


def gradient_kernel(plan, scaling, count_in, *refs):
    given, small = list(refs[:count_in]), refs[count_in]
    results, small_out = refs[count_in + 1 : count_in + 3], refs[count_in + 3]
    sums = Sums(plan, given, refs[count_in + 4 :])
    sums.greet()
    every = tuple(range(count_in))
    sums.launch_all(*every)
    sums.small_held[0] = small[...]
    sums.small_send()
    sums.finish(results, small_out, scaling, every)


def dot_nt(left, right):
    return lax.dot_general(
        left, right, (((1,), (1,)), ((), ())), preferred_element_type=jnp.float32
    )


def dot_tn(left, right):
    return lax.dot_general(
        left, right, (((0,), (0,)), ((), ())), preferred_element_type=jnp.float32
    )


def dot_nn(left, right):
    return jnp.dot(left, right, preferred_element_type=jnp.float32)


def silu_pair(values):
    sigmoid = 0.5 * jnp.tanh(0.5 * values) + 0.5
    active = values * sigmoid
    return active, sigmoid + active * (1.0 - sigmoid)


def half(value):
    return value.astype(jnp.bfloat16)


def full(value):
    return value.astype(jnp.float32)


def store_rows(target, value, low, high):
    lead = target.shape[:-2]
    target[(slice(None),) * (len(lead) + 1) + (slice(low, high),)] = half(value).reshape(
        lead + (target.shape[-2], high - low)
    )


CHUNK = 256


def chunks(low, high):
    return [slice(at, min(at + CHUNK, high)) for at in range(low, high, CHUNK)]


class Unit:
    names = ("hidden", "turned", "gate", "mark", "value", "slope", "gated", "shared", "tilt")
    names += ("query", "keyed", "raised", "spread", "pulled")

    def __init__(self, refs, win, wout, scales, gain, length):
        for name, ref in zip(self.names, refs):
            setattr(self, name, ref)
        self.win, self.wout, self.gain, self.length = win, wout, gain, length
        self.first_scale, self.second_scale = scales
        self.width = wout.shape[0]
        self.root = query_root(self.query.shape[-1])

    @staticmethod
    def scratch(rows, model, width, shared):
        wide, narrow, square = (rows, width), (rows, shared), (rows, CHUNK)
        shapes = [(rows, model), (model, rows)] + [wide] * 5
        made = [pltpu.VMEM(shape, jnp.bfloat16) for shape in shapes]
        made += [pltpu.VMEM(narrow, jnp.float32)] * 2
        made += [pltpu.VMEM(shape, jnp.bfloat16) for shape in (narrow, narrow, square, square)]
        made.append(pltpu.VMEM((rows, 2 * width + shared), jnp.bfloat16))
        return made

    def norm(self, inputs):
        hidden = half(normed(full(inputs), self.gain))
        self.hidden[...] = hidden
        self.turned[...] = hidden.T

    def project(self):
        width = self.width
        for cols in chunks(0, width):
            active, slope = silu_pair(dot_nn(self.hidden[...], self.win[:, cols]))
            self.gate[:, cols] = half(active)
            self.mark[:, cols] = half(slope)
        active, slope = silu_pair(dot_nn(self.hidden[...], self.win[:, 2 * width :]))
        self.shared[...] = active
        self.tilt[...] = slope
        self.query[...] = half(active * self.first_scale)
        self.keyed[...] = half(active * self.second_scale)
        for cols in chunks(0, width):
            from_cols = slice(width + cols.start, width + cols.stop)
            active, slope = silu_pair(dot_nn(self.hidden[...], self.win[:, from_cols]))
            self.value[:, cols] = half(active)
            self.slope[:, cols] = half(slope)

    def attend(self, rows, mask):
        raised = jnp.maximum(dot_nt(self.query[rows], self.keyed[rows]) * self.root, 0.0)
        if mask is not None:
            raised = jnp.where(mask, raised, 0.0)
        self.raised[rows] = half(raised)
        weights = half(raised * raised * (1.0 / self.length))
        self.spread[rows] = weights.T
        for cols in chunks(0, self.width):
            mixed = dot_nn(weights, self.value[rows, cols])
            self.gated[rows, cols] = half(full(self.gate[rows, cols]) * mixed)
            self.mark[rows, cols] = half(full(self.mark[rows, cols]) * mixed)

    def result(self, inputs, rows):
        return half(full(inputs) + dot_nn(self.gated[rows], self.wout[...]))

    def pull_gated(self, upstream, pulled_mix):
        for cols in chunks(0, self.width):
            pulled_mix[:, cols] = half(dot_nt(upstream, self.wout[cols, :]))

    def pull_mixer(self, rows, pulled_mix, sums):
        width = self.width
        for cols in chunks(0, width):
            grad = full(pulled_mix[rows, cols])
            self.pulled[rows, cols] = half(grad * full(self.mark[rows, cols]))
            grad_mixed = half(grad * full(self.gate[rows, cols]))
            pulled_mix[rows, cols] = grad_mixed
            grad_value = dot_nn(self.spread[rows], grad_mixed)
            to_cols = slice(width + cols.start, width + cols.stop)
            self.pulled[rows, to_cols] = half(grad_value * full(self.slope[rows, cols]))
        grad_weights = dot_nt(pulled_mix[rows], self.value[rows])
        grad_scores = half(
            grad_weights * full(self.raised[rows]) * (2.0 * self.root / self.length)
        )
        grad_query = dot_nn(grad_scores, self.keyed[rows])
        grad_keyed = dot_tn(grad_scores, self.query[rows])
        shared = self.shared[rows]
        sums[0] += jnp.sum(grad_query * shared, axis=0, keepdims=True)
        sums[1] += jnp.sum(grad_keyed * shared, axis=0, keepdims=True)
        grad_shared = grad_query * self.first_scale + grad_keyed * self.second_scale
        self.pulled[rows, 2 * width :] = half(grad_shared * self.tilt[rows])

    def pull_inputs(self, inputs, upstream, grad_hidden):
        inputs = full(inputs)
        scaled = lax.rsqrt(jnp.mean(inputs * inputs, axis=-1, keepdims=True) + EPSILON)
        unit = inputs * scaled
        gain_sum = jnp.sum(grad_hidden * unit, axis=0, keepdims=True)
        pulled = grad_hidden * self.gain
        along = jnp.mean(pulled * unit, axis=-1, keepdims=True)
        return half(full(upstream) + scaled * (pulled - unit * along)), gain_sum


def query_root(width):
    return width ** (-0.5)


LINKS = (("send_sems", 8), ("recv_sems", 8), ("load_sems", 9))


def layer_scratch(rows, model, width, shared, parts):
    blocked = (parts, 2, rows // CHUNK, CHUNK // (2 * parts), model)
    placed = (rows // CHUNK, 2, parts, CHUNK // (2 * parts), model)
    columns = 2 * width + shared
    named = {"x": (rows, model)}
    for unit in range(2):
        named[f"win{unit}"] = (model, columns)
        named[f"wout{unit}"] = (width, model)
    for name in ("firsts", "outs", "back"):
        named[name] = blocked
    for name in ("first_pos", "up", "seconds", "backs"):
        named[name] = placed
    named["pulled_mix"] = (rows, width)
    named["gated_turned"] = (width, rows)
    made = {name: pltpu.VMEM(shape, jnp.bfloat16) for name, shape in named.items()}
    made["grad_hidden"] = pltpu.VMEM((rows, model), jnp.float32)
    for name, count in LINKS:
        made[name] = pltpu.SemaphoreType.DMA((count,))
    return made


def layer_kernel(plan, scaling, names, *refs):
    x_hbm, cot_hbm, win_hbm, wout_hbm, scales, gains = refs[:6]
    results, small_out, out, back_frames = refs[6:8], refs[8], refs[9], refs[10]
    scratch = refs[11:]
    at = dict(zip(names, scratch))
    scratch = scratch[len(names) :]
    count = len(Unit.names)
    unit_refs, scratch = (scratch[:count], scratch[count : 2 * count]), scratch[2 * count :]
    grads, scratch = scratch[:4], scratch[4:]
    sums = Sums(plan, grads, scratch)
    across = axis_bits("seq")[0]
    me = lax.axis_index("seq")
    other = 1 - me
    rows = at["x"].shape[0]
    tiles = [slice(low, low + CHUNK) for low in range(0, rows, CHUNK)]
    parts = at["firsts"].shape[0]
    group = at["firsts"].shape[3]
    units = [
        Unit(
            unit_refs[k],
            at[f"win{k}"],
            at[f"wout{k}"],
            (scales[k, 0:1], scales[k, 1:2]),
            gains[k : k + 1],
            (CHUNK, 2 * parts)[k],
        )
        for k in range(2)
    ]
    early, late = units

    sources = [x_hbm, win_hbm.at[0], wout_hbm.at[0]]
    targets = [at["x"], at["win0"], at["wout0"]]
    for part in range(parts):
        sources.append(cot_hbm.at[part, me])
        targets.append(at["up"].at[:, me, part])
    sources += [wout_hbm.at[1], win_hbm.at[1]]
    targets += [at["wout1"], at["win1"]]
    loads = [
        pltpu.make_async_copy(source, target, at["load_sems"].at[spot])
        for spot, (source, target) in enumerate(zip(sources, targets))
    ]
    for load in loads:
        load.start()
    sums.greet()

    def cross(spot, source, target):
        return sums.copy(
            source, target, at["send_sems"].at[spot], at["recv_sems"].at[spot], across
        )

    ups = [
        cross(part, cot_hbm.at[part, other], at["up"].at[:, me, part]) for part in range(parts)
    ]

    loads[0].wait()
    early.norm(at["x"][...])
    loads[1].wait()
    early.project()
    loads[2].wait()
    firsts, seconds, backs = [], [], []
    for part, tile in enumerate(tiles):
        early.attend(tile, None)
        at["firsts"][part] = early.result(at["x"][tile], tile).reshape(at["firsts"].shape[1:])
        firsts.append(
            cross(parts + part, at["firsts"].at[part, other], at["first_pos"].at[:, me, part])
        )
        at["first_pos"][:, me, part] = at["firsts"][part, me]

    for load in loads[3:]:
        load.wait()
    for made in ups:
        made.wait_recv()
    upstream = at["up"][...].reshape(rows, -1)
    late.pull_gated(upstream, at["pulled_mix"])

    for made in firsts:
        made.wait_recv()
    first_pos = at["first_pos"][...].reshape(rows, -1)
    late.norm(first_pos)
    late.project()
    square = (CHUNK, CHUNK)
    mask = jnp.bitwise_and(lax.broadcasted_iota(jnp.int32, square, 0), group - 1) == (
        jnp.bitwise_and(lax.broadcasted_iota(jnp.int32, square, 1), group - 1)
    )
    for turn, tile in enumerate(tiles):
        late.attend(tile, mask)
        second = late.result(at["first_pos"][turn].reshape(CHUNK, -1), tile)
        at["seconds"][turn] = second.reshape(at["seconds"].shape[1:])
        seconds.append(
            cross(2 * parts + turn, at["seconds"].at[turn, other], at["outs"].at[:, me, turn])
        )
        at["outs"][:, me, turn] = at["seconds"][turn, me]

    def out_grads(unit, upstream, array):
        at["gated_turned"][...] = unit.gated[...].T
        for index in sums.of_arrays((array,)):
            _, low, high, _ = plan[index]
            for cols in chunks(low, high):
                value = dot_nn(at["gated_turned"][...], upstream[:, cols])
                store_rows(grads[array], value, cols.start, cols.stop)
            sums.launch(index)

    def in_grads(unit, array, between):
        for index in sums.of_arrays((array,)):
            _, low, high, _ = plan[index]
            for cols in chunks(low, high):
                value = dot_nn(unit.turned[...], unit.pulled[:, cols])
                store_rows(grads[array], value, cols.start, cols.stop)
            sums.launch(index)
            between()

    out_grads(late, upstream, 1)
    late_sums, early_sums = [0.0, 0.0], [0.0, 0.0]
    for tile in tiles:
        late.pull_mixer(tile, at["pulled_mix"], late_sums)
    sums.advance_all(1)
    at["grad_hidden"][...] = dot_nt(late.pulled[...], late.win[...])
    late_gain = 0.0
    for turn, tile in enumerate(tiles):
        back, gain_sum = late.pull_inputs(
            at["first_pos"][turn].reshape(CHUNK, -1), upstream[tile], at["grad_hidden"][tile]
        )
        late_gain += gain_sum
        at["backs"][turn] = back.reshape(at["backs"].shape[1:])
        backs.append(
            cross(3 * parts + turn, at["backs"].at[turn, other], at["back"].at[:, me, turn])
        )
        at["back"][:, me, turn] = at["backs"][turn, me]
    in_grads(late, 0, lambda: None)
    sums.advance_all(1)

    for made in backs:
        made.wait_recv()
    upstream = at["back"][...].reshape(rows, -1)
    out_grads(early, upstream, 2)
    sums.advance_all(0)
    early.pull_gated(upstream, at["pulled_mix"])
    sums.advance_all(1)
    for tile in tiles:
        early.pull_mixer(tile, at["pulled_mix"], early_sums)
        sums.advance_all(2)
    in_grads(early, 3, lambda: sums.advance_all(0))
    sums.advance_all(3)
    sums.advance_all(1)
    at["grad_hidden"][...] = dot_nt(early.pulled[...], early.win[...])
    sums.advance_all(2)
    early_gain = 0.0
    for tile in tiles:
        back, gain_sum = early.pull_inputs(at["x"][tile], upstream[tile], at["grad_hidden"][tile])
        early_gain += gain_sum
        back_frames[tile] = back
    lanes = gains.shape[-1] // 128
    for line in range(lanes):
        cols = slice(128 * line, 128 * (line + 1))
        sums.small_held[0, line : line + 1] = early_gain[:, cols]
        sums.small_held[0, lanes + line : lanes + line + 1] = late_gain[:, cols]
    for line, value in enumerate(early_sums + late_sums):
        sums.small_held[0, 2 * lanes + line : 2 * lanes + line + 1] = value
    sums.small_send()
    for made in seconds:
        made.wait_recv()
    out[...] = at["outs"][...]
    sums.finish(results, small_out, scaling, (3,), (2, 0, 1))


def wide_shape(rows, columns):
    steps = len(axis_bits("dp")) + len(axis_bits("seq"))
    return (2,) * steps + (rows >> steps, columns)


def sums_outputs(wide, lines):
    shapes = [
        jax.ShapeDtypeStruct((2, lax.axis_size("seq")) + shape[-2:], jnp.float32)
        for shape in wide[:2]
    ]
    return shapes + [jax.ShapeDtypeStruct(lines, jnp.float32)]


def reduced(partials, cuts, small, scaling):
    wide = [wide_shape(*partial.shape) for partial in partials]
    lines = small.reshape(-1, 128)
    space = pl.BlockSpec(memory_space=pltpu.VMEM)
    outs = sums_outputs(wide, lines.shape)
    made = pl.pallas_call(
        partial_of(gradient_kernel, cuts, scaling, len(partials)),
        out_shape=outs,
        in_specs=[space] * (len(partials) + 1),
        out_specs=[space] * len(outs),
        scratch_shapes=sums_scratch(cuts, wide, lines.shape),
        compiler_params=pltpu.CompilerParams(
            collective_id=0, has_side_effects=True, vmem_limit_bytes=24 << 20
        ),
        name="gradient_sums",
    )(*[value.reshape(shape) for value, shape in zip(partials, wide)], lines)
    sums = [value.reshape(2, -1, value.shape[-1]) for value in made[:2]]
    return sums, made[2].reshape(-1)


def whole_layer(frames, cotangent, weight_in, qk_scales, weight_out, gains, cuts, scaling):
    rows, model = frames.shape[0] * frames.shape[1], frames.shape[2]
    width, columns = weight_out.shape[1], weight_in.shape[2]
    shared = qk_scales.shape[-1]
    parts = rows // BLOCK
    blocked = (parts, 2, rows // CHUNK, CHUNK // (2 * parts), model)
    wide = [wide_shape(*pair) for pair in ((model, columns), (width, model)) * 2]
    wide[2], wide[3] = wide[3], wide[2]
    lines = (2 * model // 128 + 4 * shared // 128, 128)
    named = layer_scratch(rows, model, width, shared, parts)
    vmem, any_space = (
        pl.BlockSpec(memory_space=pltpu.VMEM),
        pl.BlockSpec(memory_space=pl.ANY),
    )
    outs = sums_outputs(wide, lines) + [
        jax.ShapeDtypeStruct(blocked, jnp.bfloat16),
        jax.ShapeDtypeStruct((rows, model), jnp.bfloat16),
    ]
    made = pl.pallas_call(
        partial_of(layer_kernel, cuts, scaling, tuple(named)),
        out_shape=outs,
        in_specs=[any_space] * 4 + [vmem] * 2,
        out_specs=[vmem] * len(outs),
        scratch_shapes=list(named.values())
        + Unit.scratch(rows, model, width, shared) * 2
        + [pltpu.VMEM(shape, jnp.bfloat16) for shape in wide]
        + sums_scratch(cuts, wide, lines),
        compiler_params=pltpu.CompilerParams(
            collective_id=0, has_side_effects=True, vmem_limit_bytes=58 << 20
        ),
        name="layer_step",
    )(
        frames.reshape(rows, model),
        cotangent.reshape(blocked),
        weight_in,
        weight_out,
        qk_scales,
        gains,
    )
    sums = [value.reshape(2, -1, value.shape[-1]) for value in made[:2]]
    return sums, made[2].reshape(-1), made[3], made[4]


def exchange(value, split, join):
    count = lax.axis_size("seq")
    me = lax.axis_index("seq")
    piece = value.shape[split] // count
    width = value.shape[join]
    shape = list(value.shape)
    shape[split] = piece
    shape[join] = width * count
    if count == 2:
        halves = jnp.split(value, 2, axis=split)
        own = jnp.where(me == 0, halves[0], halves[1])
        got = lax.ppermute(jnp.where(me == 0, halves[1], halves[0]), "seq", [(0, 1), (1, 0)])
        return jnp.concatenate(
            [jnp.where(me == 0, own, got), jnp.where(me == 0, got, own)], axis=join
        )
    out = jnp.zeros(shape, value.dtype)
    for step in range(count):
        other = jnp.bitwise_xor(me, step)
        part = lax.dynamic_slice_in_dim(value, other * piece, piece, split)
        if step:
            part = lax.ppermute(part, "seq", [(i, i ^ step) for i in range(count)])
        out = lax.dynamic_update_slice_in_dim(out, part, other * width, join)
    return out


def column_cuts(columns, parts):
    lanes = columns // 128
    ends = [128 * ((lanes * (i + 1)) // parts) for i in range(parts)]
    return list(zip([0] + ends[:-1], ends))


def column_cuts(columns, parts):
    grains = -(-columns // CHUNK)
    ends = [min(columns, CHUNK * ((grains * (i + 1)) // parts)) for i in range(parts)]
    return list(zip([0] + ends[:-1], ends))


CUTS = ((3, (0, 1, 2)), (2, (0, 2)), (2, (1, 0)), (3, (0, 2, 1)))


def on_device(frames, cotangent, weight_in, qk_scales, weight_out, gains):
    block_count = frames.shape[1] // BLOCK
    width = frames.shape[2]
    ways = lax.axis_size("seq")
    tokens_all = frames.shape[0] * frames.shape[1] * lax.axis_size("dp") * ways
    scaling = tokens_all ** (-0.5)
    cuts = []
    shapes = [weight_in.shape[2], width, width, weight_in.shape[2]]
    for array, (parts, turns) in enumerate(CUTS):
        for (low, high), turn in zip(column_cuts(shapes[array], parts), turns):
            cuts.append((array, low, high, turn))
    steps = len(axis_bits("dp")) + len(axis_bits("seq"))
    fits = (width >> steps) % 16 == 0 and ways == 2 and block_count == 2 and frames.shape[0] == 1
    if fits:
        sums, small, result, back_frames = whole_layer(
            frames, cotangent, weight_in, qk_scales, weight_out, gains, cuts, scaling
        )
    else:
        blocked = frames.reshape(-1, BLOCK, width)
        upstream = exchange(cotangent.reshape(block_count, BLOCK, width), 1, 0)
        first, saved_first = unit_forward(
            blocked, weight_in[0], qk_scales[0], weight_out[0], gains[0], 1
        )
        first_pos = exchange(first, 1, 0)
        second, saved_second = unit_forward(
            first_pos, weight_in[1], qk_scales[1], weight_out[1], gains[1], 0
        )
        result = exchange(second, 0, 1)
        back_pos, *late = unit_backward(
            first_pos,
            upstream,
            weight_in[1],
            qk_scales[1],
            weight_out[1],
            gains[1],
            saved_second,
            0,
        )
        back_frames, *early = unit_backward(
            blocked,
            exchange(back_pos, 0, 1),
            weight_in[0],
            qk_scales[0],
            weight_out[0],
            gains[0],
            saved_first,
            1,
        )
        packed = jnp.concatenate(
            [early[2], late[2], early[3].reshape(-1), late[3].reshape(-1)]
        )
        grads = [value.astype(jnp.bfloat16) for value in (late[0], late[1], early[1], early[0])]
        sums, small = reduced(grads, cuts, packed, scaling)
    return (
        result.reshape(frames.shape),
        back_frames.reshape(frames.shape),
        sums[0],
        sums[1],
        small[: 2 * width].reshape(2, width),
        small[2 * width :].reshape(qk_scales.shape),
    )


def solution(mesh):
    in_specs = (P("dp", "seq", None), P("dp", "seq", None), P(), P(), P(), P())
    out_specs = (
        P("dp", "seq", None),
        P("dp", "seq", None),
        P(None, "dp", None),
        P(None, "dp", None),
        P(),
        P(),
    )
    return jax.shard_map(
        on_device, mesh=mesh, in_specs=in_specs, out_specs=out_specs, check_vma=False
    )
```

```python
from functools import partial
from functools import partial as partial_of
from types import SimpleNamespace

import jax
import jax.numpy as jnp
from jax import lax
from jax.experimental import pallas as pl
from jax.experimental.pallas import tpu as pltpu
from jax.sharding import PartitionSpec as P

BLOCK = 256


EPSILON = 1e-06


def normed(values, gain_row):
    scaling = lax.rsqrt(jnp.mean(values * values, axis=-1, keepdims=True) + EPSILON)
    return values * scaling * gain_row


def mixer(projected, scale_pair, attend_axis):
    width = (projected.shape[-1] - scale_pair.shape[-1]) // 2
    active = jax.nn.silu(projected)
    gate_part = active[..., :width]
    value_part = active[..., width : 2 * width].astype(jnp.bfloat16)
    shared = active[..., 2 * width :]
    query = (shared * scale_pair[0]).astype(jnp.bfloat16)
    keyed = (shared * scale_pair[1]).astype(jnp.bfloat16)
    length = projected.shape[attend_axis]
    if attend_axis == 1:
        score_form = "gls,gms->glm"
        mix_form = "glm,gme->gle"
    else:
        score_form = "lgs,mgs->glm"
        mix_form = "glm,mge->lge"
    scores = jnp.einsum(score_form, query, keyed, preferred_element_type=jnp.float32)
    scores = scores * scale_pair.shape[-1] ** (-0.5)
    weights = (jnp.square(jax.nn.relu(scores)) / length).astype(jnp.bfloat16)
    mixed = jnp.einsum(mix_form, weights, value_part, preferred_element_type=jnp.float32)
    return (gate_part * mixed).astype(jnp.bfloat16)


def rows_product(left, right):
    left_rows = left.reshape(-1, left.shape[-1])
    right_rows = right.reshape(-1, right.shape[-1])
    return lax.dot_general(
        left_rows, right_rows, (((0,), (0,)), ((), ())), preferred_element_type=jnp.float32
    )


def against(values, weight):
    return lax.dot_general(
        values, weight, (((values.ndim - 1,), (1,)), ((), ())), preferred_element_type=jnp.float32
    )


def unit_forward(inputs_now, weight_in, scale_pair, weight_out, gain_row, attend_axis):
    hidden = normed(inputs_now.astype(jnp.float32), gain_row).astype(jnp.bfloat16)
    projected = jnp.dot(hidden, weight_in, preferred_element_type=jnp.float32)
    gated = mixer(projected, scale_pair, attend_axis)
    result = (
        inputs_now.astype(jnp.float32)
        + jnp.dot(gated, weight_out, preferred_element_type=jnp.float32)
    ).astype(jnp.bfloat16)
    return (result, (hidden, projected, gated))


def unit_backward(
    inputs_now, upstream, weight_in, scale_pair, weight_out, gain_row, saved, attend_axis
):
    hidden, projected, gated = saved
    grad_out = rows_product(gated, upstream)
    grad_gated = against(upstream, weight_out).astype(jnp.bfloat16)
    pulled = jax.vjp(partial(mixer, attend_axis=attend_axis), projected, scale_pair)[1]
    grad_proj, grad_scale = pulled(grad_gated)
    grad_proj = grad_proj.astype(jnp.bfloat16)
    grad_in = rows_product(hidden, grad_proj)
    grad_hidden = against(grad_proj, weight_in)
    norm_pull = jax.vjp(normed, inputs_now.astype(jnp.float32), gain_row)[1]
    grad_inputs, grad_gain = norm_pull(grad_hidden)
    grad_inputs = (upstream.astype(jnp.float32) + grad_inputs).astype(jnp.bfloat16)
    return (grad_inputs, grad_in, grad_out, grad_gain, grad_scale)


def bit_of(axis, bit):
    return lax.rem(lax.axis_index(axis) // (1 << bit), 2)


def axis_bits(axis):
    return [(axis, bit) for bit in range(lax.axis_size(axis).bit_length() - 1)]


def partner(axis, bit):
    spot = {name: lax.axis_index(name) for name in ("dp", "seq")}
    spot[axis] = spot[axis] + (1 << bit) * (1 - 2 * bit_of(axis, bit))
    return (spot["dp"], spot["seq"])


def halving_order(turn):
    dp_bits, seq_bits = axis_bits("dp"), axis_bits("seq")
    rest = dp_bits[1:2] + seq_bits + dp_bits[2:-1]
    turn = turn % max(len(rest), 1)
    return dp_bits[:1] + rest[turn:] + rest[:turn] + dp_bits[2:][-1:]


def order_of(turn):
    if not isinstance(turn, str):
        return halving_order(turn)
    named = dict(zip("cxzwy", axis_bits("dp") + axis_bits("seq")))
    return [named[letter] for letter in "c" + turn]


def joined_last(turn):
    return isinstance(turn, str) and turn.endswith("y")


def place_of(known, leading):
    return tuple(known.get(bit, slice(None)) for bit in leading)


SLOTS = ((0, 1), (1, 1), (1, 0), (0, 0))


class Sums:
    def __init__(self, plan, given, buffers, results, scaling):
        self.plan, self.given = plan, given
        self.small_held, self.small_got, self.sends, self.recvs = buffers[:4]
        buffers = buffers[4:]
        self.dp_bits, self.seq_bits = axis_bits("dp"), axis_bits("seq")
        self.leading = self.dp_bits[::-1] + self.seq_bits[::-1]
        self.steps = len(self.leading)
        total = len(plan)
        self.accs, self.gathers = buffers[:total], buffers[total : 2 * total]
        self.landings = [
            buffers[2 * total + self.steps * i : 2 * total + self.steps * (i + 1)]
            for i in range(total)
        ]
        self.mine = {bit: bit_of(*bit) for bit in self.leading}
        self.where = {bit: partner(*bit) for bit in self.leading}
        self.orders = [order_of(turn) for _, _, _, turn in plan]
        self.joined = [joined_last(turn) for _, _, _, turn in plan]
        self.small_order = self.leading
        self.results, self.scaling = results, scaling
        self.settled = [False] * total
        self.flying = [None] * total
        self.known = [{} for _ in plan]
        self.at_step = [0] * total
        self.started = []
        self.small_step = 0

    def greet(self):
        barrier = pltpu.get_barrier_semaphore()
        for bit in self.leading:
            pl.semaphore_signal(
                barrier, inc=1, device_id=self.where[bit], device_id_type=pl.DeviceIdType.MESH
            )

    def greeted(self):
        pl.semaphore_wait(pltpu.get_barrier_semaphore(), self.steps)

    def copy(self, source, target, send_sem, recv_sem, bit):
        made = pltpu.make_async_remote_copy(
            src_ref=source,
            dst_ref=target,
            send_sem=send_sem,
            recv_sem=recv_sem,
            device_id=self.where[bit],
            device_id_type=pl.DeviceIdType.MESH,
        )
        made.start()
        self.started.append(made)
        return made

    def send(self, source, target, row, column, bit):
        return self.copy(
            source, target, self.sends.at[row, column], self.recvs.at[row, column], bit
        )

    def launch(self, index, step=0):
        array, low, high, _ = self.plan[index]
        order = self.orders[index]
        bit = order[step]
        if step == 0:
            place = place_of({bit: 1 - self.mine[bit]}, self.leading)
            source = self.given[array].at[place + (slice(None), slice(low, high))]
        else:
            left = [other for other in self.leading if other != order[0]]
            known = dict(self.known[index])
            if not (self.joined[index] and step == self.steps - 1):
                known[bit] = 1 - self.mine[bit]
            source = self.accs[index].at[place_of(known, left)]
        self.flying[index] = self.send(source, self.landings[index][step], index, step, bit)

    def advance(self, index):
        step = self.at_step[index]
        if step >= self.steps:
            return self.settle(index)
        array, low, high, _ = self.plan[index]
        order = self.orders[index]
        bit = order[step]
        self.flying[index].wait_recv()
        landed = self.landings[index][step]
        left = [other for other in self.leading if other != order[0]]
        acc = self.accs[index]
        self.at_step[index] = step + 1
        if self.joined[index] and step == self.steps - 1:
            self.gathers[index][...] = acc[place_of(self.known[index], left)] + landed[...]
            return self.settle(index)
        if step == 0:
            place = place_of({bit: self.mine[bit]}, self.leading)
            acc[...] = self.given[array][place + (slice(None), slice(low, high))] + landed[...]
        else:
            self.known[index][bit] = self.mine[bit]
            place = place_of(self.known[index], left)
            acc[place] = acc[place] + landed[...]
        if step + 1 < self.steps:
            self.launch(index, step + 1)
        else:
            spot = place_of(self.mine, self.seq_bits)
            self.gathers[index][spot] = acc[place_of(self.mine, left)]
            if self.seq_bits:
                held = self.gathers[index].at[spot]
                self.flying[index] = self.send(held, held, index, self.steps, self.seq_bits[0])

    def settle(self, index):
        if self.settled[index]:
            return
        self.settled[index] = True
        array, low, high, _ = self.plan[index]
        if not self.joined[index]:
            for turn in range(len(self.seq_bits)):
                self.flying[index].wait_recv()
                if turn + 1 < len(self.seq_bits):
                    have = {bit: self.mine[bit] for bit in self.seq_bits[turn + 1 :]}
                    spot = self.gathers[index].at[place_of(have, self.seq_bits)]
                    self.flying[index] = self.send(
                        spot, spot, index, self.steps + turn + 1, self.seq_bits[turn + 1]
                    )
        for part in range(1 << len(self.seq_bits)):
            spot = tuple((part >> bit) % 2 for _, bit in self.seq_bits)
            place, unit = SLOTS[array]
            self.results[place][unit, part, :, low:high] = (
                full(self.gathers[index][spot]) * self.scaling
            )

    def of_arrays(self, wanted):
        return [index for index, (array, _, _, _) in enumerate(self.plan) if array in wanted]

    def launch_all(self, *wanted):
        for index in self.of_arrays(wanted):
            self.launch(index)

    def advance_all(self, *wanted):
        for index in self.of_arrays(wanted):
            self.advance(index)

    def small_send(self):
        step = self.small_step
        self.small_copy = self.send(
            self.small_held.at[step],
            self.small_got.at[step],
            len(self.plan),
            step,
            self.small_order[step],
        )

    def small_advance(self):
        step = self.small_step
        if step >= self.steps:
            return
        self.small_copy.wait_recv()
        self.small_held[step + 1] = self.small_held[step] + self.small_got[step]
        self.small_step = step + 1
        if step + 1 < self.steps:
            self.small_send()

    def take(self, indices):
        for index in indices:
            if index == len(self.plan):
                self.small_advance()
            else:
                self.advance(index)

    def finish(self, small_out):
        total = len(self.plan)
        while min(self.at_step) < self.steps or self.small_step < self.steps:
            self.take(
                [index for index in range(total) if self.at_step[index] < self.steps] + [total]
            )
        self.take(range(total))
        small_out[...] = self.small_held[self.steps] * self.scaling
        for made in self.started:
            made.wait_send()


def sums_scratch(cuts, wide, lines):
    dp_bits, seq_bits = axis_bits("dp"), axis_bits("seq")
    steps = len(dp_bits) + len(seq_bits)
    accs, gathers, landings = [], [], []
    for array, low, high, turn in cuts:
        tail = (wide[array][-2], high - low)
        accs.append(pltpu.VMEM((2,) * (steps - 1) + tail, jnp.bfloat16))
        gathers.append(pltpu.VMEM((2,) * len(seq_bits) + tail, jnp.bfloat16))
        folds = [steps - 1 - step for step in range(steps)]
        if joined_last(turn):
            folds[-1] += 1
        landings += [pltpu.VMEM((2,) * fold + tail, jnp.bfloat16) for fold in folds]
    sems = pltpu.SemaphoreType.DMA((len(cuts) + 1, steps + len(seq_bits)))
    return [
        pltpu.VMEM((steps + 1,) + lines, jnp.float32),
        pltpu.VMEM((steps,) + lines, jnp.float32),
        sems,
        sems,
    ] + accs + gathers + landings


def gradient_kernel(plan, scaling, count_in, *refs):
    given, small = list(refs[:count_in]), refs[count_in]
    results, small_out = refs[count_in + 1 : count_in + 3], refs[count_in + 3]
    sums = Sums(plan, given, refs[count_in + 4 :], results, scaling)
    sums.greet()
    sums.greeted()
    every = tuple(range(count_in))
    sums.launch_all(*every)
    sums.small_held[0] = small[...]
    sums.small_send()
    sums.finish(small_out)


def dot_nt(left, right):
    return lax.dot_general(
        left, right, (((1,), (1,)), ((), ())), preferred_element_type=jnp.float32
    )


def dot_tn(left, right):
    return lax.dot_general(
        left, right, (((0,), (0,)), ((), ())), preferred_element_type=jnp.float32
    )


def dot_nn(left, right):
    return jnp.dot(left, right, preferred_element_type=jnp.float32)


def silu_pair(values):
    sigmoid = 0.5 * jnp.tanh(0.5 * values) + 0.5
    active = values * sigmoid
    return active, sigmoid + active * (1.0 - sigmoid)


def half(value):
    return value.astype(jnp.bfloat16)


def full(value):
    return value.astype(jnp.float32)


def store_rows(target, value, low, high):
    lead = target.shape[:-2]
    target[(slice(None),) * (len(lead) + 1) + (slice(low, high),)] = half(value).reshape(
        lead + (target.shape[-2], high - low)
    )


CHUNK = 256
WIDE = 512


def chunks(low, high, grain=CHUNK):
    ends = list(range(low + grain, high - grain // 2, grain)) + [high]
    return [slice(at, end) for at, end in zip([low] + ends[:-1], ends)]


class Unit:
    names = ("hidden", "turned", "gate", "mark", "value", "slope", "gated", "shared", "tilt")
    names += ("query", "keyed", "raised", "spread", "pulled")

    def __init__(self, refs, win, wout, scales, gain, length):
        for name, ref in zip(self.names, refs):
            setattr(self, name, ref)
        self.win, self.wout, self.gain, self.length = win, wout, gain, length
        self.first_scale, self.second_scale = scales
        self.width = wout.shape[0]
        self.root = query_root(self.query.shape[-1])

    @staticmethod
    def scratch(rows, model, width, shared):
        wide, narrow, square = (rows, width), (rows, shared), (rows, CHUNK)
        shapes = [(rows, model), (model, rows)] + [wide] * 5
        made = [pltpu.VMEM(shape, jnp.bfloat16) for shape in shapes]
        made += [pltpu.VMEM(narrow, jnp.float32)] * 2
        made += [pltpu.VMEM(shape, jnp.bfloat16) for shape in (narrow, narrow, square, square)]
        made.append(pltpu.VMEM((rows, 2 * width + shared), jnp.bfloat16))
        return made

    def norm(self, inputs, rows):
        hidden = half(normed(full(inputs), self.gain))
        self.hidden[rows] = hidden
        self.turned[:, rows] = hidden.T

    def project(self, rows, loads=()):
        width = self.width
        if loads:
            loads[0].wait()
        for cols in chunks(0, width):
            active, slope = silu_pair(dot_nn(self.hidden[rows], self.win[:, cols]))
            self.gate[rows, cols] = half(active)
            self.mark[rows, cols] = half(slope)
        if loads:
            loads[1].wait()
        active, slope = silu_pair(dot_nn(self.hidden[rows], self.win[:, 2 * width :]))
        self.shared[rows] = active
        self.tilt[rows] = slope
        self.query[rows] = half(active * self.first_scale)
        self.keyed[rows] = half(active * self.second_scale)
        if loads:
            loads[2].wait()
        for cols in chunks(0, width):
            from_cols = slice(width + cols.start, width + cols.stop)
            active, slope = silu_pair(dot_nn(self.hidden[rows], self.win[:, from_cols]))
            self.value[rows, cols] = half(active)
            self.slope[rows, cols] = half(slope)

    def attend(self, rows, mask):
        raised = jnp.maximum(dot_nt(self.query[rows], self.keyed[rows]) * self.root, 0.0)
        if mask is not None:
            raised = jnp.where(mask, raised, 0.0)
        self.raised[rows] = half(raised)
        weights = half(raised * raised * (1.0 / self.length))
        self.spread[rows] = weights.T
        for cols in chunks(0, self.width):
            mixed = dot_nn(weights, self.value[rows, cols])
            self.gated[rows, cols] = half(full(self.gate[rows, cols]) * mixed)
            self.mark[rows, cols] = half(full(self.mark[rows, cols]) * mixed)

    def result(self, inputs, rows):
        return half(full(inputs) + dot_nn(self.gated[rows], self.wout[...]))

    def pull_gated(self, upstream, rows, pulled_mix):
        for cols in chunks(0, self.width):
            pulled_mix[rows, cols] = half(dot_nt(upstream, self.wout[cols, :]))

    def pull_mixer(self, rows, pulled_mix, sums):
        width = self.width
        for cols in chunks(0, width):
            grad = full(pulled_mix[rows, cols])
            self.pulled[rows, cols] = half(grad * full(self.mark[rows, cols]))
            grad_mixed = half(grad * full(self.gate[rows, cols]))
            pulled_mix[rows, cols] = grad_mixed
            grad_value = dot_nn(self.spread[rows], grad_mixed)
            to_cols = slice(width + cols.start, width + cols.stop)
            self.pulled[rows, to_cols] = half(grad_value * full(self.slope[rows, cols]))
        grad_weights = dot_nt(pulled_mix[rows], self.value[rows])
        grad_scores = half(
            grad_weights * full(self.raised[rows]) * (2.0 * self.root / self.length)
        )
        grad_query = dot_nn(grad_scores, self.keyed[rows])
        grad_keyed = dot_tn(grad_scores, self.query[rows])
        shared = self.shared[rows]
        sums[0] += jnp.sum(grad_query * shared, axis=0, keepdims=True)
        sums[1] += jnp.sum(grad_keyed * shared, axis=0, keepdims=True)
        grad_shared = grad_query * self.first_scale + grad_keyed * self.second_scale
        self.pulled[rows, 2 * width :] = half(grad_shared * self.tilt[rows])

    def pull_inputs(self, inputs, upstream, grad_hidden):
        inputs = full(inputs)
        scaled = lax.rsqrt(jnp.mean(inputs * inputs, axis=-1, keepdims=True) + EPSILON)
        unit = inputs * scaled
        gain_sum = jnp.sum(grad_hidden * unit, axis=0, keepdims=True)
        pulled = grad_hidden * self.gain
        along = jnp.mean(pulled * unit, axis=-1, keepdims=True)
        return half(full(upstream) + scaled * (pulled - unit * along)), gain_sum


def query_root(width):
    return width ** (-0.5)


LINKS = (("send_sems", 12), ("recv_sems", 12), ("load_sems", 11))


def layer_scratch(rows, model, width, shared, parts):
    blocked = (parts, 2, rows // CHUNK, CHUNK // (2 * parts), model)
    placed = (rows // CHUNK, 2, parts, CHUNK // (2 * parts), model)
    columns = 2 * width + shared
    named = {"x": (rows, model)}
    for unit in range(2):
        named[f"win{unit}"] = (model, columns)
        named[f"wout{unit}"] = (width, model)
    for name in ("firsts", "outs", "back"):
        named[name] = blocked
    for name in ("first_pos", "up", "seconds", "backs"):
        named[name] = placed
    named["pulled_mix"] = (rows, width)
    named["gated_turned"] = (width, rows)
    made = {name: pltpu.VMEM(shape, jnp.bfloat16) for name, shape in named.items()}
    made["grad_hidden"] = pltpu.VMEM((rows, model), jnp.float32)
    made["scales"] = pltpu.VMEM((2, 2, shared), jnp.float32)
    made["gains"] = pltpu.VMEM((2, model), jnp.float32)
    for name, count in LINKS:
        made[name] = pltpu.SemaphoreType.DMA((count,))
    return made


def layer_kernel(plan, scaling, names, *refs):
    x_hbm, cot_hbm, win_hbm, wout_hbm, scales_hbm, gains_hbm = refs[:6]
    results, small_out, out, back_frames = refs[6:8], refs[8], refs[9], refs[10]
    scratch = refs[11:]
    at = SimpleNamespace(**dict(zip(names, scratch)))
    scratch = scratch[len(names) :]
    count = len(Unit.names)
    unit_refs, scratch = (scratch[:count], scratch[count : 2 * count]), scratch[2 * count :]
    grads, scratch = scratch[:4], scratch[4:]
    sums = Sums(plan, grads, scratch, results, scaling)
    sums.small_order = order_of("xyzw")
    across = axis_bits("seq")[0]
    me = lax.axis_index("seq")
    other = 1 - me
    rows = at.x.shape[0]
    tiles = [slice(low, low + CHUNK) for low in range(0, rows, CHUNK)]
    parts = at.firsts.shape[0]
    group = at.firsts.shape[3]
    scales, gains = at.scales, at.gains
    width = wout_hbm.shape[1]
    sources = [x_hbm, gains_hbm, scales_hbm]
    targets = [at.x, gains, scales]
    for cols in (slice(0, width), slice(2 * width, None), slice(width, 2 * width)):
        sources.append(win_hbm.at[0, :, cols])
        targets.append(at.win0.at[:, cols])
    sources.append(wout_hbm.at[0])
    targets.append(at.wout0)
    for part in range(parts):
        sources.append(cot_hbm.at[part, me])
        targets.append(at.up.at[:, me, part])
    sources += [wout_hbm.at[1], win_hbm.at[1]]
    targets += [at.wout1, at.win1]
    loads = [
        pltpu.make_async_copy(source, target, at.load_sems.at[spot])
        for spot, (source, target) in enumerate(zip(sources, targets))
    ]
    for load in loads[:7]:
        load.start()
    sums.greet()
    def cross(spot, source, target):
        return sums.copy(
            source, target, at.send_sems.at[spot], at.recv_sems.at[spot], across
        )

    def send_up(turn, part):
        return cross(
            4 + 2 * turn + part, cot_hbm.at[part, other, turn], at.up.at[turn, me, part]
        )

    for load in loads[:3]:
        load.wait()
    units = [
        Unit(
            unit_refs[k],
            (at.win0, at.win1)[k],
            (at.wout0, at.wout1)[k],
            (scales[k, 0:1], scales[k, 1:2]),
            gains[k : k + 1],
            (CHUNK, 2 * parts)[k],
        )
        for k in range(2)
    ]
    early, late = units

    firsts = {}

    def send_first(part, turn):
        firsts[part, turn] = cross(
            parts * part + turn,
            at.firsts.at[part, other, turn],
            at.first_pos.at[turn, me, part],
        )

    seconds = {}

    def take(name):
        for turn, place in enumerate(SECONDS_AT):
            if place == name:
                seconds[turn] = cross(
                    8 + turn, at.seconds.at[turn, other], at.outs.at[:, me, turn]
                )
        sums.take(HOOKS.get(name, ()))

    turns = range(len(tiles))
    for part, tile in enumerate(tiles):
        early.norm(at.x[tile], tile)
        if part == 0:
            for load in loads[7:]:
                load.start()
        early.project(tile, loads[3:6] if part == 0 else ())
        if part == 0:
            sums.greeted()
            ups = [[send_up(0, 0)]]
        early.attend(tile, None)
        if part == 0:
            loads[6].wait()
        at.firsts[part] = early.result(at.x[tile], tile).reshape(
            at.firsts.shape[1:]
        )
        send_first(part, 0)
        at.first_pos[:, me, part] = at.firsts[part, me]
    for load in loads[7:]:
        load.wait()
    firsts[1, 0].wait_send()
    sums.started = [made for made in sums.started if made is not firsts[1, 0]]
    ups[0].append(send_up(0, 1))
    for part in range(parts):
        send_first(part, 1)

    def launch_ready(array, low, high):
        for index in sums.of_arrays((array,)):
            if low < plan[index][2] <= high:
                sums.launch(index)

    def out_grads(unit, upstream, array, name):
        at.gated_turned[...] = unit.gated[...].T
        for turn, cols in enumerate(chunks(0, upstream.shape[-1], WIDE)):
            value = dot_nn(at.gated_turned[...], upstream[:, cols])
            store_rows(grads[array], value, cols.start, cols.stop)
            launch_ready(array, cols.start, cols.stop)
            take(f"{name}{turn}")

    def in_grads(unit, array, name):
        for turn, cols in enumerate(chunks(0, unit.pulled.shape[-1], WIDE)):
            value = dot_nn(unit.turned[...], unit.pulled[:, cols])
            store_rows(grads[array], value, cols.start, cols.stop)
            launch_ready(array, cols.start, cols.stop)
            take(f"{name}{turn}")

    square = (CHUNK, CHUNK)
    mask = jnp.bitwise_and(lax.broadcasted_iota(jnp.int32, square, 0), group - 1) == (
        jnp.bitwise_and(lax.broadcasted_iota(jnp.int32, square, 1), group - 1)
    )
    late_sums, early_sums = [0.0, 0.0], [0.0, 0.0]
    late_gain, early_gain = 0.0, 0.0
    backs = []
    for turn, tile in enumerate(tiles):
        for part in range(parts):
            firsts[part, turn].wait_recv()
        inputs = at.first_pos[turn].reshape(CHUNK, -1)
        late.norm(inputs, tile)
        if turn == 0:
            ups.append([send_up(1, part) for part in range(parts)])
        late.project(tile)
        late.attend(tile, mask)
        at.seconds[turn] = late.result(inputs, tile).reshape(at.seconds.shape[1:])
        at.outs[:, me, turn] = at.seconds[turn, me]
        for made in ups[turn]:
            made.wait_recv()
        upstream = at.up[turn].reshape(CHUNK, -1)
        if turn == 1 and LATE_FIRST == "P":
            out_grads(late, at.up[...].reshape(rows, -1), 1, "o")
        late.pull_gated(upstream, tile, at.pulled_mix)
        late.pull_mixer(tile, at.pulled_mix, late_sums)
        grad_hidden = dot_nt(late.pulled[tile], late.win[...])
        back, gain_sum = late.pull_inputs(inputs, upstream, grad_hidden)
        late_gain += gain_sum
        at.backs[turn] = back.reshape(at.backs.shape[1:])
        backs.append(cross(10 + turn, at.backs.at[turn, other], at.back.at[:, me, turn]))
        at.back[:, me, turn] = at.backs[turn, me]

    take("h")
    if LATE_FIRST == "R":
        out_grads(late, at.up[...].reshape(rows, -1), 1, "o")
    in_grads(late, 0, "i")
    if LATE_FIRST == "Q":
        out_grads(late, at.up[...].reshape(rows, -1), 1, "o")
    take("wb")
    for made in backs:
        made.wait_recv()
    upstream = at.back[...].reshape(rows, -1)
    if EARLY_OUT_FIRST:
        out_grads(early, upstream, 2, "q")
    early.pull_gated(upstream, slice(0, rows), at.pulled_mix)
    take("pg")
    for turn, tile in enumerate(tiles):
        early.pull_mixer(tile, at.pulled_mix, early_sums)
        take(f"p{turn}")
    in_grads(early, 3, "j")
    if not EARLY_OUT_FIRST:
        out_grads(early, upstream, 2, "q")
    model = upstream.shape[-1]
    for turn, cols in enumerate(chunks(0, model)):
        at.grad_hidden[:, cols] = dot_nt(early.pulled[...], early.win[cols, :])
        take(f"d{turn}")
    for tile in tiles:
        back, gain_sum = early.pull_inputs(at.x[tile], upstream[tile], at.grad_hidden[tile])
        early_gain += gain_sum
        back_frames[tile] = back
    lanes = model // 128
    for line in range(lanes):
        cols = slice(128 * line, 128 * (line + 1))
        sums.small_held[0, line : line + 1] = early_gain[:, cols]
        sums.small_held[0, lanes + line : lanes + line + 1] = late_gain[:, cols]
    for line, value in enumerate(early_sums + late_sums):
        sums.small_held[0, 2 * lanes + line : 2 * lanes + line + 1] = value
    sums.small_send()
    take("x")
    later = 2 * len(TAIL) // 3
    sums.take(TAIL[:later])
    for made in seconds.values():
        made.wait_recv()
    out[...] = at.outs[...]
    sums.take(TAIL[later:])
    sums.finish(small_out)


def handing_kernel(gin, gout, lines, out, back, out_to, back_to, gin_to, gout_to, gains, scales, sems):
    pairs = ((gin, gin_to), (gout, gout_to), (out, out_to), (back, back_to))
    copies = [
        pltpu.make_async_copy(source, target, sems.at[spot])
        for spot, (source, target) in enumerate(pairs)
    ]
    for made in copies:
        made.start()
    lanes = gains.shape[1] // 128
    for line in range(2 * lanes):
        unit, at = divmod(line, lanes)
        gains[unit : unit + 1, 128 * at : 128 * (at + 1)] = lines[line : line + 1]
    scales[0] = lines[2 * lanes : 2 * lanes + 2]
    scales[1] = lines[2 * lanes + 2 : 2 * lanes + 4]
    for made in copies:
        made.wait()


def wide_shape(rows, columns):
    steps = len(axis_bits("dp")) + len(axis_bits("seq"))
    return (2,) * steps + (rows >> steps, columns)


def sums_outputs(wide, lines):
    shapes = [
        jax.ShapeDtypeStruct((2, lax.axis_size("seq")) + shape[-2:], jnp.float32)
        for shape in wide[:2]
    ]
    return shapes + [jax.ShapeDtypeStruct(lines, jnp.float32)]


def reduced(partials, cuts, small, scaling):
    wide = [wide_shape(*partial.shape) for partial in partials]
    lines = small.reshape(-1, 128)
    space = pl.BlockSpec(memory_space=pltpu.VMEM)
    outs = sums_outputs(wide, lines.shape)
    made = pl.pallas_call(
        partial_of(gradient_kernel, cuts, scaling, len(partials)),
        out_shape=outs,
        in_specs=[space] * (len(partials) + 1),
        out_specs=[space] * len(outs),
        scratch_shapes=sums_scratch(cuts, wide, lines.shape),
        compiler_params=pltpu.CompilerParams(
            collective_id=0, has_side_effects=True, vmem_limit_bytes=24 << 20
        ),
        name="gradient_sums",
    )(*[value.reshape(shape) for value, shape in zip(partials, wide)], lines)
    sums = [value.reshape(2, -1, value.shape[-1]) for value in made[:2]]
    return sums, made[2].reshape(-1)


def whole_layer(frames, cotangent, weight_in, qk_scales, weight_out, gains, cuts, scaling):
    rows, model = frames.shape[0] * frames.shape[1], frames.shape[2]
    width, columns = weight_out.shape[1], weight_in.shape[2]
    shared = qk_scales.shape[-1]
    parts = rows // BLOCK
    blocked = (parts, 2, rows // CHUNK, CHUNK // (2 * parts), model)
    wide = [wide_shape(*pair) for pair in ((model, columns), (width, model)) * 2]
    wide[2], wide[3] = wide[3], wide[2]
    lines = (2 * model // 128 + 4 * shared // 128, 128)
    named = layer_scratch(rows, model, width, shared, parts)
    vmem, any_space = (
        pl.BlockSpec(memory_space=pltpu.VMEM),
        pl.BlockSpec(memory_space=pl.ANY),
    )
    outs = sums_outputs(wide, lines) + [
        jax.ShapeDtypeStruct(blocked, jnp.bfloat16),
        jax.ShapeDtypeStruct((rows, model), jnp.bfloat16),
    ]
    outs = [pltpu.VMEM(value.shape, value.dtype) for value in outs]
    made = pl.pallas_call(
        partial_of(layer_kernel, cuts, scaling, tuple(named)),
        out_shape=outs,
        in_specs=[any_space] * 6,
        out_specs=[vmem] * len(outs),
        scratch_shapes=list(named.values())
        + Unit.scratch(rows, model, width, shared) * 2
        + [pltpu.VMEM(shape, jnp.bfloat16) for shape in wide]
        + sums_scratch(cuts, wide, lines),
        compiler_params=pltpu.CompilerParams(
            collective_id=0, has_side_effects=True, vmem_limit_bytes=62 << 20
        ),
        name="layer_step",
    )(
        *[
            pltpu.with_memory_space_constraint(value, pltpu.HBM)
            for value in (
                frames.reshape(rows, model),
                cotangent.reshape(blocked),
                weight_in,
                weight_out,
                qk_scales,
                gains,
            )
        ]
    )
    handed = [made[3], made[4], made[0], made[1]]
    gin, gout, lines, out, back = made
    out, back, gin, gout, gain_sums, scale_sums = pl.pallas_call(
        handing_kernel,
        out_shape=[jax.ShapeDtypeStruct(value.shape, value.dtype) for value in handed]
        + [
            jax.ShapeDtypeStruct(gains.shape, jnp.float32),
            jax.ShapeDtypeStruct(qk_scales.shape, jnp.float32),
        ],
        in_specs=[vmem] * 5,
        out_specs=[any_space] * 4 + [vmem] * 2,
        scratch_shapes=[pltpu.SemaphoreType.DMA((4,))],
        compiler_params=pltpu.CompilerParams(vmem_limit_bytes=4 << 20),
        name="handing",
    )(gin, gout, lines, out, back)
    sums = [value.reshape(2, -1, value.shape[-1]) for value in (gin, gout)]
    return out, back, *sums, gain_sums, scale_sums


def exchange(value, split, join):
    count = lax.axis_size("seq")
    me = lax.axis_index("seq")
    piece = value.shape[split] // count
    width = value.shape[join]
    shape = list(value.shape)
    shape[split] = piece
    shape[join] = width * count
    if count == 2:
        halves = jnp.split(value, 2, axis=split)
        own = jnp.where(me == 0, halves[0], halves[1])
        got = lax.ppermute(jnp.where(me == 0, halves[1], halves[0]), "seq", [(0, 1), (1, 0)])
        return jnp.concatenate(
            [jnp.where(me == 0, own, got), jnp.where(me == 0, got, own)], axis=join
        )
    out = jnp.zeros(shape, value.dtype)
    for step in range(count):
        other = jnp.bitwise_xor(me, step)
        part = lax.dynamic_slice_in_dim(value, other * piece, piece, split)
        if step:
            part = lax.ppermute(part, "seq", [(i, i ^ step) for i in range(count)])
        out = lax.dynamic_update_slice_in_dim(out, part, other * width, join)
    return out


def column_cuts(columns, parts):
    lanes = columns // 128
    ends = [128 * ((lanes * (i + 1)) // parts) for i in range(parts)]
    return list(zip([0] + ends[:-1], ends))


def column_cuts(columns, parts):
    grains = -(-columns // CHUNK)
    ends = [min(columns, CHUNK * ((grains * (i + 1)) // parts)) for i in range(parts)]
    return list(zip([0] + ends[:-1], ends))


CUTS = (
    (0, 0, 512, "xzyw"),
    (0, 512, 1024, "zxwy"),
    (0, 1024, 1536, "xzwy"),
    (0, 1536, 2176, "zxyw"),
    (1, 0, 256, "xywz"),
    (1, 256, 512, "zxyw"),
    (2, 0, 256, "xywz"),
    (2, 256, 512, "zyxw"),
    (3, 0, 384, "yxwz"),
    (3, 384, 768, "xyzw"),
    (3, 768, 1152, "yxzw"),
    (3, 1152, 1536, "zxwy"),
    (3, 1536, 1920, "yxzw"),
    (3, 1920, 2176, "yzxw"),
)

HOOKS = {
    "h": (4,),
    "i0": (5,),
    "wb": (0, 1, 2, 3),
    "pg": (4,),
    "p0": (5,),
    "j3": (0,),
    "q0": (1, 8, 9, 4, 10),
    "d0": (11, 12, 13),
    "d1": (2,),
    "x": (6, 3, 7),
}

SECONDS_AT = ('h', 'p1')

LATE_FIRST = "P"
EARLY_OUT_FIRST = False

TAIL = (
    5, 0, 14, 1, 8, 4, 9, 11, 10, 2, 6, 12, 13, 7, 3, 14, 5, 4, 0, 8, 1, 9, 11, 13, 10, 2, 6, 5,
    12, 0, 7, 9, 13, 3, 8, 14, 10, 4, 11, 1, 12, 2, 7, 5, 6, 0, 9, 13, 8, 14, 11, 3, 10, 12, 6,
    9, 13, 7, 8, 14, 3, 10, 12, 6, 7,
)


def plain_cuts(columns, model):
    cuts = []
    for array, (extent, parts) in enumerate(((columns, 3), (model, 2), (model, 2), (columns, 3))):
        for turn, (low, high) in enumerate(column_cuts(extent, parts)):
            cuts.append((array, low, high, turn + array))
    return cuts


def on_device(frames, cotangent, weight_in, qk_scales, weight_out, gains):
    block_count = frames.shape[1] // BLOCK
    width = frames.shape[2]
    ways = lax.axis_size("seq")
    tokens_all = frames.shape[0] * frames.shape[1] * lax.axis_size("dp") * ways
    scaling = tokens_all ** (-0.5)
    steps = len(axis_bits("dp")) + len(axis_bits("seq"))
    fits = (width >> steps) % 16 == 0 and ways == 2 and lax.axis_size("dp") == 16
    fits = fits and block_count == 2 and frames.shape[0] == 1
    fits = fits and weight_in.shape[2] == CUTS[-1][2]
    if fits:
        result, back_frames, *sums, gain_sums, scale_sums = whole_layer(
            frames, cotangent, weight_in, qk_scales, weight_out, gains, CUTS, scaling
        )
    else:
        blocked = frames.reshape(-1, BLOCK, width)
        upstream = exchange(cotangent.reshape(block_count, BLOCK, width), 1, 0)
        first, saved_first = unit_forward(
            blocked, weight_in[0], qk_scales[0], weight_out[0], gains[0], 1
        )
        first_pos = exchange(first, 1, 0)
        second, saved_second = unit_forward(
            first_pos, weight_in[1], qk_scales[1], weight_out[1], gains[1], 0
        )
        result = exchange(second, 0, 1)
        back_pos, *late = unit_backward(
            first_pos,
            upstream,
            weight_in[1],
            qk_scales[1],
            weight_out[1],
            gains[1],
            saved_second,
            0,
        )
        back_frames, *early = unit_backward(
            blocked,
            exchange(back_pos, 0, 1),
            weight_in[0],
            qk_scales[0],
            weight_out[0],
            gains[0],
            saved_first,
            1,
        )
        packed = jnp.concatenate(
            [early[2], late[2], early[3].reshape(-1), late[3].reshape(-1)]
        )
        grads = [value.astype(jnp.bfloat16) for value in (late[0], late[1], early[1], early[0])]
        cuts = plain_cuts(weight_in.shape[2], width)
        sums, small = reduced(grads, cuts, packed, scaling)
        gain_sums = small[: 2 * width].reshape(2, width)
        scale_sums = small[2 * width :].reshape(qk_scales.shape)
    return (
        result.reshape(frames.shape),
        back_frames.reshape(frames.shape),
        sums[0],
        sums[1],
        gain_sums,
        scale_sums,
    )


def solution(mesh):
    in_specs = (P("dp", "seq", None), P("dp", "seq", None), P(), P(), P(), P())
    out_specs = (
        P("dp", "seq", None),
        P("dp", "seq", None),
        P(None, "dp", None),
        P(None, "dp", None),
        P(),
        P(),
    )
    return jax.shard_map(
        on_device, mesh=mesh, in_specs=in_specs, out_specs=out_specs, check_vma=False
    )
```

```python
from functools import partial
from functools import partial as partial_of
from types import SimpleNamespace

import jax
import jax.numpy as jnp
from jax import lax
from jax.experimental import pallas as pl
from jax.experimental.pallas import tpu as pltpu
from jax.sharding import PartitionSpec as P

BLOCK = 256


EPSILON = 1e-06


def normed(values, gain_row):
    scaling = lax.rsqrt(jnp.mean(values * values, axis=-1, keepdims=True) + EPSILON)
    return values * scaling * gain_row


def mixer(projected, scale_pair, attend_axis):
    width = (projected.shape[-1] - scale_pair.shape[-1]) // 2
    active = jax.nn.silu(projected)
    gate_part = active[..., :width]
    value_part = active[..., width : 2 * width].astype(jnp.bfloat16)
    shared = active[..., 2 * width :]
    query = (shared * scale_pair[0]).astype(jnp.bfloat16)
    keyed = (shared * scale_pair[1]).astype(jnp.bfloat16)
    length = projected.shape[attend_axis]
    if attend_axis == 1:
        score_form = "gls,gms->glm"
        mix_form = "glm,gme->gle"
    else:
        score_form = "lgs,mgs->glm"
        mix_form = "glm,mge->lge"
    scores = jnp.einsum(score_form, query, keyed, preferred_element_type=jnp.float32)
    scores = scores * scale_pair.shape[-1] ** (-0.5)
    weights = (jnp.square(jax.nn.relu(scores)) / length).astype(jnp.bfloat16)
    mixed = jnp.einsum(mix_form, weights, value_part, preferred_element_type=jnp.float32)
    return (gate_part * mixed).astype(jnp.bfloat16)


def rows_product(left, right):
    left_rows = left.reshape(-1, left.shape[-1])
    right_rows = right.reshape(-1, right.shape[-1])
    return lax.dot_general(
        left_rows, right_rows, (((0,), (0,)), ((), ())), preferred_element_type=jnp.float32
    )


def against(values, weight):
    return lax.dot_general(
        values, weight, (((values.ndim - 1,), (1,)), ((), ())), preferred_element_type=jnp.float32
    )


def unit_forward(inputs_now, weight_in, scale_pair, weight_out, gain_row, attend_axis):
    hidden = normed(inputs_now.astype(jnp.float32), gain_row).astype(jnp.bfloat16)
    projected = jnp.dot(hidden, weight_in, preferred_element_type=jnp.float32)
    gated = mixer(projected, scale_pair, attend_axis)
    result = (
        inputs_now.astype(jnp.float32)
        + jnp.dot(gated, weight_out, preferred_element_type=jnp.float32)
    ).astype(jnp.bfloat16)
    return (result, (hidden, projected, gated))


def unit_backward(
    inputs_now, upstream, weight_in, scale_pair, weight_out, gain_row, saved, attend_axis
):
    hidden, projected, gated = saved
    grad_out = rows_product(gated, upstream)
    grad_gated = against(upstream, weight_out).astype(jnp.bfloat16)
    pulled = jax.vjp(partial(mixer, attend_axis=attend_axis), projected, scale_pair)[1]
    grad_proj, grad_scale = pulled(grad_gated)
    grad_proj = grad_proj.astype(jnp.bfloat16)
    grad_in = rows_product(hidden, grad_proj)
    grad_hidden = against(grad_proj, weight_in)
    norm_pull = jax.vjp(normed, inputs_now.astype(jnp.float32), gain_row)[1]
    grad_inputs, grad_gain = norm_pull(grad_hidden)
    grad_inputs = (upstream.astype(jnp.float32) + grad_inputs).astype(jnp.bfloat16)
    return (grad_inputs, grad_in, grad_out, grad_gain, grad_scale)


def bit_of(axis, bit):
    return lax.rem(lax.axis_index(axis) // (1 << bit), 2)


def axis_bits(axis):
    return [(axis, bit) for bit in range(lax.axis_size(axis).bit_length() - 1)]


def partner(axis, bit):
    spot = {name: lax.axis_index(name) for name in ("dp", "seq")}
    spot[axis] = spot[axis] + (1 << bit) * (1 - 2 * bit_of(axis, bit))
    return (spot["dp"], spot["seq"])


def halving_order(turn):
    dp_bits, seq_bits = axis_bits("dp"), axis_bits("seq")
    rest = dp_bits[1:2] + seq_bits + dp_bits[2:-1]
    turn = turn % max(len(rest), 1)
    return dp_bits[:1] + rest[turn:] + rest[:turn] + dp_bits[2:][-1:]


def order_of(turn):
    if not isinstance(turn, str):
        return halving_order(turn)
    named = dict(zip("cxzwy", axis_bits("dp") + axis_bits("seq")))
    return [named[letter] for letter in "c" + turn]


def joined_last(turn):
    return isinstance(turn, str) and turn.endswith("y")


def place_of(known, leading):
    return tuple(known.get(bit, slice(None)) for bit in leading)


SLOTS = ((0, 1), (1, 1), (1, 0), (0, 0))


class Sums:
    def __init__(self, plan, given, buffers, results, scaling):
        self.plan, self.given = plan, given
        self.small_held, self.small_got, self.sends, self.recvs = buffers[:4]
        buffers = buffers[4:]
        self.dp_bits, self.seq_bits = axis_bits("dp"), axis_bits("seq")
        self.leading = self.dp_bits[::-1] + self.seq_bits[::-1]
        self.steps = len(self.leading)
        total = len(plan)
        self.accs, self.gathers = buffers[:total], buffers[total : 2 * total]
        self.landings = [
            buffers[2 * total + self.steps * i : 2 * total + self.steps * (i + 1)]
            for i in range(total)
        ]
        self.mine = {bit: bit_of(*bit) for bit in self.leading}
        self.where = {bit: partner(*bit) for bit in self.leading}
        self.orders = [order_of(turn) for _, _, _, turn in plan]
        self.joined = [joined_last(turn) for _, _, _, turn in plan]
        self.small_order = self.leading
        self.results, self.scaling = results, scaling
        self.settled = [False] * total
        self.flying = [None] * total
        self.known = [{} for _ in plan]
        self.at_step = [0] * total
        self.started = []
        self.small_step = 0

    def greet(self):
        barrier = pltpu.get_barrier_semaphore()
        for bit in self.leading:
            pl.semaphore_signal(
                barrier, inc=1, device_id=self.where[bit], device_id_type=pl.DeviceIdType.MESH
            )

    def greeted(self):
        pl.semaphore_wait(pltpu.get_barrier_semaphore(), self.steps)

    def copy(self, source, target, send_sem, recv_sem, bit):
        made = pltpu.make_async_remote_copy(
            src_ref=source,
            dst_ref=target,
            send_sem=send_sem,
            recv_sem=recv_sem,
            device_id=self.where[bit],
            device_id_type=pl.DeviceIdType.MESH,
        )
        made.start()
        self.started.append(made)
        return made

    def send(self, source, target, row, column, bit):
        return self.copy(
            source, target, self.sends.at[row, column], self.recvs.at[row, column], bit
        )

    def launch(self, index, step=0):
        array, low, high, _ = self.plan[index]
        order = self.orders[index]
        bit = order[step]
        if step == 0:
            place = place_of({bit: 1 - self.mine[bit]}, self.leading)
            source = self.given[array].at[place + (slice(None), slice(low, high))]
        else:
            left = [other for other in self.leading if other != order[0]]
            known = dict(self.known[index])
            if not (self.joined[index] and step == self.steps - 1):
                known[bit] = 1 - self.mine[bit]
            source = self.accs[index].at[place_of(known, left)]
        self.flying[index] = self.send(source, self.landings[index][step], index, step, bit)

    def advance(self, index):
        step = self.at_step[index]
        if step >= self.steps:
            return self.settle(index)
        array, low, high, _ = self.plan[index]
        order = self.orders[index]
        bit = order[step]
        self.flying[index].wait_recv()
        landed = self.landings[index][step]
        left = [other for other in self.leading if other != order[0]]
        acc = self.accs[index]
        self.at_step[index] = step + 1
        if self.joined[index] and step == self.steps - 1:
            self.gathers[index][...] = acc[place_of(self.known[index], left)] + landed[...]
            return self.settle(index)
        if step == 0:
            place = place_of({bit: self.mine[bit]}, self.leading)
            acc[...] = self.given[array][place + (slice(None), slice(low, high))] + landed[...]
        else:
            self.known[index][bit] = self.mine[bit]
            place = place_of(self.known[index], left)
            acc[place] = acc[place] + landed[...]
        if step + 1 < self.steps:
            self.launch(index, step + 1)
        else:
            spot = place_of(self.mine, self.seq_bits)
            self.gathers[index][spot] = acc[place_of(self.mine, left)]
            if self.seq_bits:
                held = self.gathers[index].at[spot]
                self.flying[index] = self.send(held, held, index, self.steps, self.seq_bits[0])

    def settle(self, index):
        if self.settled[index]:
            return
        self.settled[index] = True
        array, low, high, _ = self.plan[index]
        if not self.joined[index]:
            for turn in range(len(self.seq_bits)):
                self.flying[index].wait_recv()
                if turn + 1 < len(self.seq_bits):
                    have = {bit: self.mine[bit] for bit in self.seq_bits[turn + 1 :]}
                    spot = self.gathers[index].at[place_of(have, self.seq_bits)]
                    self.flying[index] = self.send(
                        spot, spot, index, self.steps + turn + 1, self.seq_bits[turn + 1]
                    )
        for part in range(1 << len(self.seq_bits)):
            spot = tuple((part >> bit) % 2 for _, bit in self.seq_bits)
            place, unit = SLOTS[array]
            self.results[place][unit, part, :, low:high] = (
                full(self.gathers[index][spot]) * self.scaling
            )

    def of_arrays(self, wanted):
        return [index for index, (array, _, _, _) in enumerate(self.plan) if array in wanted]

    def launch_all(self, *wanted):
        for index in self.of_arrays(wanted):
            self.launch(index)

    def advance_all(self, *wanted):
        for index in self.of_arrays(wanted):
            self.advance(index)

    def small_send(self):
        step = self.small_step
        self.small_copy = self.send(
            self.small_held.at[step],
            self.small_got.at[step],
            len(self.plan),
            step,
            self.small_order[step],
        )

    def small_advance(self):
        step = self.small_step
        if step >= self.steps:
            return
        self.small_copy.wait_recv()
        self.small_held[step + 1] = self.small_held[step] + self.small_got[step]
        self.small_step = step + 1
        if step + 1 < self.steps:
            self.small_send()

    def take(self, indices):
        for index in indices:
            if index == len(self.plan):
                self.small_advance()
            else:
                self.advance(index)

    def finish(self, small_out):
        total = len(self.plan)
        while min(self.at_step) < self.steps or self.small_step < self.steps:
            self.take(
                [index for index in range(total) if self.at_step[index] < self.steps] + [total]
            )
        self.take(range(total))
        small_out[...] = self.small_held[self.steps] * self.scaling
        for made in self.started:
            made.wait_send()


def sums_scratch(cuts, wide, lines):
    dp_bits, seq_bits = axis_bits("dp"), axis_bits("seq")
    steps = len(dp_bits) + len(seq_bits)
    accs, gathers, landings = [], [], []
    for array, low, high, turn in cuts:
        tail = (wide[array][-2], high - low)
        accs.append(pltpu.VMEM((2,) * (steps - 1) + tail, jnp.bfloat16))
        gathers.append(pltpu.VMEM((2,) * len(seq_bits) + tail, jnp.bfloat16))
        folds = [steps - 1 - step for step in range(steps)]
        if joined_last(turn):
            folds[-1] += 1
        landings += [pltpu.VMEM((2,) * fold + tail, jnp.bfloat16) for fold in folds]
    sems = pltpu.SemaphoreType.DMA((len(cuts) + 1, steps + len(seq_bits)))
    return [
        pltpu.VMEM((steps + 1,) + lines, jnp.float32),
        pltpu.VMEM((steps,) + lines, jnp.float32),
        sems,
        sems,
    ] + accs + gathers + landings


def gradient_kernel(plan, scaling, count_in, *refs):
    given, small = list(refs[:count_in]), refs[count_in]
    results, small_out = refs[count_in + 1 : count_in + 3], refs[count_in + 3]
    sums = Sums(plan, given, refs[count_in + 4 :], results, scaling)
    sums.greet()
    sums.greeted()
    every = tuple(range(count_in))
    sums.launch_all(*every)
    sums.small_held[0] = small[...]
    sums.small_send()
    sums.finish(small_out)


def dot_nt(left, right):
    return lax.dot_general(
        left, right, (((1,), (1,)), ((), ())), preferred_element_type=jnp.float32
    )


def dot_tn(left, right):
    return lax.dot_general(
        left, right, (((0,), (0,)), ((), ())), preferred_element_type=jnp.float32
    )


def dot_nn(left, right):
    return jnp.dot(left, right, preferred_element_type=jnp.float32)


def silu_pair(values):
    sigmoid = 0.5 * jnp.tanh(0.5 * values) + 0.5
    active = values * sigmoid
    return active, sigmoid + active * (1.0 - sigmoid)


def half(value):
    return value.astype(jnp.bfloat16)


def full(value):
    return value.astype(jnp.float32)


def store_rows(target, value, low, high):
    lead = target.shape[:-2]
    target[(slice(None),) * (len(lead) + 1) + (slice(low, high),)] = half(value).reshape(
        lead + (target.shape[-2], high - low)
    )


CHUNK = 256
WIDE = 512


def chunks(low, high, grain=CHUNK):
    ends = list(range(low + grain, high - grain // 2, grain)) + [high]
    return [slice(at, end) for at, end in zip([low] + ends[:-1], ends)]


class Unit:
    names = ("hidden", "turned", "gate", "mark", "value", "slope", "gated", "shared", "tilt")
    names += ("query", "keyed", "raised", "spread", "pulled")

    def __init__(self, refs, win, wout, scales, gain, length):
        for name, ref in zip(self.names, refs):
            setattr(self, name, ref)
        self.win, self.wout, self.gain, self.length = win, wout, gain, length
        self.first_scale, self.second_scale = scales
        self.width = wout.shape[0]
        self.root = query_root(self.query.shape[-1])

    @staticmethod
    def scratch(rows, model, width, shared):
        wide, narrow, square = (rows, width), (rows, shared), (rows, CHUNK)
        shapes = [(rows, model), (model, rows)] + [wide] * 5
        made = [pltpu.VMEM(shape, jnp.bfloat16) for shape in shapes]
        made += [pltpu.VMEM(narrow, jnp.float32)] * 2
        made += [pltpu.VMEM(shape, jnp.bfloat16) for shape in (narrow, narrow, square, square)]
        made.append(pltpu.VMEM((rows, 2 * width + shared), jnp.bfloat16))
        return made

    def norm(self, inputs, rows):
        hidden = half(normed(full(inputs), self.gain))
        self.hidden[rows] = hidden
        self.turned[:, rows] = hidden.T

    def project(self, rows, loads=()):
        width = self.width
        if loads:
            loads[0].wait()
        for cols in chunks(0, width):
            active, slope = silu_pair(dot_nn(self.hidden[rows], self.win[:, cols]))
            self.gate[rows, cols] = half(active)
            self.mark[rows, cols] = half(slope)
        if loads:
            loads[1].wait()
        active, slope = silu_pair(dot_nn(self.hidden[rows], self.win[:, 2 * width :]))
        self.shared[rows] = active
        self.tilt[rows] = slope
        self.query[rows] = half(active * self.first_scale)
        self.keyed[rows] = half(active * self.second_scale)
        if loads:
            loads[2].wait()
        for cols in chunks(0, width):
            from_cols = slice(width + cols.start, width + cols.stop)
            active, slope = silu_pair(dot_nn(self.hidden[rows], self.win[:, from_cols]))
            self.value[rows, cols] = half(active)
            self.slope[rows, cols] = half(slope)

    def attend(self, rows, mask):
        raised = jnp.maximum(dot_nt(self.query[rows], self.keyed[rows]) * self.root, 0.0)
        if mask is not None:
            raised = jnp.where(mask, raised, 0.0)
        self.raised[rows] = half(raised)
        weights = half(raised * raised * (1.0 / self.length))
        self.spread[rows] = weights.T
        for cols in chunks(0, self.width):
            mixed = dot_nn(weights, self.value[rows, cols])
            self.gated[rows, cols] = half(full(self.gate[rows, cols]) * mixed)
            self.mark[rows, cols] = half(full(self.mark[rows, cols]) * mixed)

    def result(self, inputs, rows):
        return half(full(inputs) + dot_nn(self.gated[rows], self.wout[...]))

    def pull_gated(self, upstream, rows, pulled_mix):
        for cols in chunks(0, self.width):
            pulled_mix[rows, cols] = half(dot_nt(upstream, self.wout[cols, :]))

    def pull_mixer(self, rows, pulled_mix, sums):
        width = self.width
        for cols in chunks(0, width):
            grad = full(pulled_mix[rows, cols])
            self.pulled[rows, cols] = half(grad * full(self.mark[rows, cols]))
            grad_mixed = half(grad * full(self.gate[rows, cols]))
            pulled_mix[rows, cols] = grad_mixed
            grad_value = dot_nn(self.spread[rows], grad_mixed)
            to_cols = slice(width + cols.start, width + cols.stop)
            self.pulled[rows, to_cols] = half(grad_value * full(self.slope[rows, cols]))
        grad_weights = dot_nt(pulled_mix[rows], self.value[rows])
        grad_scores = half(
            grad_weights * full(self.raised[rows]) * (2.0 * self.root / self.length)
        )
        grad_query = dot_nn(grad_scores, self.keyed[rows])
        grad_keyed = dot_tn(grad_scores, self.query[rows])
        shared = self.shared[rows]
        sums[0] += jnp.sum(grad_query * shared, axis=0, keepdims=True)
        sums[1] += jnp.sum(grad_keyed * shared, axis=0, keepdims=True)
        grad_shared = grad_query * self.first_scale + grad_keyed * self.second_scale
        self.pulled[rows, 2 * width :] = half(grad_shared * self.tilt[rows])

    def pull_inputs(self, inputs, upstream, grad_hidden):
        inputs = full(inputs)
        scaled = lax.rsqrt(jnp.mean(inputs * inputs, axis=-1, keepdims=True) + EPSILON)
        unit = inputs * scaled
        gain_sum = jnp.sum(grad_hidden * unit, axis=0, keepdims=True)
        pulled = grad_hidden * self.gain
        along = jnp.mean(pulled * unit, axis=-1, keepdims=True)
        return half(full(upstream) + scaled * (pulled - unit * along)), gain_sum


def query_root(width):
    return width ** (-0.5)


LINKS = (("send_sems", 12), ("recv_sems", 12), ("load_sems", 11))


def layer_scratch(rows, model, width, shared, parts):
    blocked = (parts, 2, rows // CHUNK, CHUNK // (2 * parts), model)
    placed = (rows // CHUNK, 2, parts, CHUNK // (2 * parts), model)
    columns = 2 * width + shared
    named = {"x": (rows, model)}
    for unit in range(2):
        named[f"win{unit}"] = (model, columns)
        named[f"wout{unit}"] = (width, model)
    for name in ("firsts", "outs", "back"):
        named[name] = blocked
    for name in ("first_pos", "up", "seconds", "backs"):
        named[name] = placed
    named["pulled_mix"] = (rows, width)
    named["gated_turned"] = (width, rows)
    made = {name: pltpu.VMEM(shape, jnp.bfloat16) for name, shape in named.items()}
    made["grad_hidden"] = pltpu.VMEM((rows, model), jnp.float32)
    made["scales"] = pltpu.VMEM((2, 2, shared), jnp.float32)
    made["gains"] = pltpu.VMEM((2, model), jnp.float32)
    for name, count in LINKS:
        made[name] = pltpu.SemaphoreType.DMA((count,))
    return made


def layer_kernel(plan, scaling, names, *refs):
    x_hbm, cot_hbm, win_hbm, wout_hbm, scales_hbm, gains_hbm = refs[:6]
    results, small_out, out, back_frames = refs[6:8], refs[8], refs[9], refs[10]
    scratch = refs[11:]
    at = SimpleNamespace(**dict(zip(names, scratch)))
    scratch = scratch[len(names) :]
    count = len(Unit.names)
    unit_refs, scratch = (scratch[:count], scratch[count : 2 * count]), scratch[2 * count :]
    grads, scratch = scratch[:4], scratch[4:]
    sums = Sums(plan, grads, scratch, results, scaling)
    sums.small_order = order_of("xyzw")
    across = axis_bits("seq")[0]
    me = lax.axis_index("seq")
    other = 1 - me
    rows = at.x.shape[0]
    tiles = [slice(low, low + CHUNK) for low in range(0, rows, CHUNK)]
    parts = at.firsts.shape[0]
    group = at.firsts.shape[3]
    scales, gains = at.scales, at.gains
    width = wout_hbm.shape[1]
    sources = [x_hbm, gains_hbm, scales_hbm]
    targets = [at.x, gains, scales]
    for cols in (slice(0, width), slice(2 * width, None), slice(width, 2 * width)):
        sources.append(win_hbm.at[0, :, cols])
        targets.append(at.win0.at[:, cols])
    sources.append(wout_hbm.at[0])
    targets.append(at.wout0)
    for part in range(parts):
        sources.append(cot_hbm.at[part, me])
        targets.append(at.up.at[:, me, part])
    sources += [wout_hbm.at[1], win_hbm.at[1]]
    targets += [at.wout1, at.win1]
    loads = [
        pltpu.make_async_copy(source, target, at.load_sems.at[spot])
        for spot, (source, target) in enumerate(zip(sources, targets))
    ]
    for load in loads[:7]:
        load.start()
    sums.greet()
    def cross(spot, source, target):
        return sums.copy(
            source, target, at.send_sems.at[spot], at.recv_sems.at[spot], across
        )

    def send_up(turn, part):
        return cross(
            4 + 2 * turn + part, cot_hbm.at[part, other, turn], at.up.at[turn, me, part]
        )

    for load in loads[:3]:
        load.wait()
    units = [
        Unit(
            unit_refs[k],
            (at.win0, at.win1)[k],
            (at.wout0, at.wout1)[k],
            (scales[k, 0:1], scales[k, 1:2]),
            gains[k : k + 1],
            (CHUNK, 2 * parts)[k],
        )
        for k in range(2)
    ]
    early, late = units

    firsts = {}

    def send_first(part, turn):
        firsts[part, turn] = cross(
            parts * part + turn,
            at.firsts.at[part, other, turn],
            at.first_pos.at[turn, me, part],
        )

    seconds = {}

    def take(name):
        for turn, place in enumerate(SECONDS_AT):
            if place == name:
                seconds[turn] = cross(
                    8 + turn, at.seconds.at[turn, other], at.outs.at[:, me, turn]
                )
        sums.take(HOOKS.get(name, ()))

    turns = range(len(tiles))
    for part, tile in enumerate(tiles):
        early.norm(at.x[tile], tile)
        if part == 0:
            for load in loads[7:]:
                load.start()
        early.project(tile, loads[3:6] if part == 0 else ())
        if part == 0:
            sums.greeted()
            ups = [[send_up(0, 0)]]
        early.attend(tile, None)
        if part == 0:
            loads[6].wait()
        at.firsts[part] = early.result(at.x[tile], tile).reshape(
            at.firsts.shape[1:]
        )
        send_first(part, 0)
        at.first_pos[:, me, part] = at.firsts[part, me]
    for load in loads[7:]:
        load.wait()
    firsts[1, 0].wait_send()
    sums.started = [made for made in sums.started if made is not firsts[1, 0]]
    ups[0].append(send_up(0, 1))
    for part in range(parts):
        send_first(part, 1)

    def launch_ready(array, low, high):
        for index in sums.of_arrays((array,)):
            if low < plan[index][2] <= high:
                sums.launch(index)

    def out_grads(unit, upstream, array, name):
        at.gated_turned[...] = unit.gated[...].T
        for turn, cols in enumerate(chunks(0, upstream.shape[-1], WIDE)):
            value = dot_nn(at.gated_turned[...], upstream[:, cols])
            store_rows(grads[array], value, cols.start, cols.stop)
            launch_ready(array, cols.start, cols.stop)
            take(f"{name}{turn}")

    def in_grads(unit, array, name):
        for turn, cols in enumerate(chunks(0, unit.pulled.shape[-1], WIDE)):
            value = dot_nn(unit.turned[...], unit.pulled[:, cols])
            store_rows(grads[array], value, cols.start, cols.stop)
            launch_ready(array, cols.start, cols.stop)
            take(f"{name}{turn}")

    square = (CHUNK, CHUNK)
    mask = jnp.bitwise_and(lax.broadcasted_iota(jnp.int32, square, 0), group - 1) == (
        jnp.bitwise_and(lax.broadcasted_iota(jnp.int32, square, 1), group - 1)
    )
    late_sums, early_sums = [0.0, 0.0], [0.0, 0.0]
    late_gain, early_gain = 0.0, 0.0
    backs = []
    for turn, tile in enumerate(tiles):
        for part in range(parts):
            firsts[part, turn].wait_recv()
        inputs = at.first_pos[turn].reshape(CHUNK, -1)
        late.norm(inputs, tile)
        if turn == 0:
            ups.append([send_up(1, part) for part in range(parts)])
        late.project(tile)
        late.attend(tile, mask)
        at.seconds[turn] = late.result(inputs, tile).reshape(at.seconds.shape[1:])
        at.outs[:, me, turn] = at.seconds[turn, me]
        for made in ups[turn]:
            made.wait_recv()
        upstream = at.up[turn].reshape(CHUNK, -1)
        if turn == 1 and LATE_FIRST == "P":
            out_grads(late, at.up[...].reshape(rows, -1), 1, "o")
        late.pull_gated(upstream, tile, at.pulled_mix)
        late.pull_mixer(tile, at.pulled_mix, late_sums)
        grad_hidden = dot_nt(late.pulled[tile], late.win[...])
        back, gain_sum = late.pull_inputs(inputs, upstream, grad_hidden)
        late_gain += gain_sum
        at.backs[turn] = back.reshape(at.backs.shape[1:])
        backs.append(cross(10 + turn, at.backs.at[turn, other], at.back.at[:, me, turn]))
        at.back[:, me, turn] = at.backs[turn, me]

    take("h")
    if LATE_FIRST == "R":
        out_grads(late, at.up[...].reshape(rows, -1), 1, "o")
    in_grads(late, 0, "i")
    if LATE_FIRST == "Q":
        out_grads(late, at.up[...].reshape(rows, -1), 1, "o")
    take("wb")
    for made in backs:
        made.wait_recv()
    upstream = at.back[...].reshape(rows, -1)
    if EARLY_OUT_FIRST:
        out_grads(early, upstream, 2, "q")
    early.pull_gated(upstream, slice(0, rows), at.pulled_mix)
    take("pg")
    for turn, tile in enumerate(tiles):
        early.pull_mixer(tile, at.pulled_mix, early_sums)
        take(f"p{turn}")
    in_grads(early, 3, "j")
    if not EARLY_OUT_FIRST:
        out_grads(early, upstream, 2, "q")
    model = upstream.shape[-1]
    for turn, cols in enumerate(chunks(0, model)):
        at.grad_hidden[:, cols] = dot_nt(early.pulled[...], early.win[cols, :])
        take(f"d{turn}")
    for tile in tiles:
        back, gain_sum = early.pull_inputs(at.x[tile], upstream[tile], at.grad_hidden[tile])
        early_gain += gain_sum
        back_frames[tile] = back
    lanes = model // 128
    for line in range(lanes):
        cols = slice(128 * line, 128 * (line + 1))
        sums.small_held[0, line : line + 1] = early_gain[:, cols]
        sums.small_held[0, lanes + line : lanes + line + 1] = late_gain[:, cols]
    for line, value in enumerate(early_sums + late_sums):
        sums.small_held[0, 2 * lanes + line : 2 * lanes + line + 1] = value
    sums.small_send()
    take("x")
    later = 2 * len(TAIL) // 3
    sums.take(TAIL[:later])
    for made in seconds.values():
        made.wait_recv()
    out[...] = at.outs[...]
    sums.take(TAIL[later:])
    sums.finish(small_out)


def handing_kernel(*refs):
    gin, gout, lines, out, back = refs[:5]
    out_to, back_to, gin_to, gout_to, gains_to, scales_to, gains, scales, sems = refs[5:]
    lanes = gains.shape[1] // 128
    pairs = []
    for source, target in ((gin, gin_to), (out, out_to), (gout, gout_to)):
        pairs += [(source.at[i], target.at[i]) for i in range(source.shape[0])]
    middle = back.shape[0] // 2
    for rows in (pl.ds(0, middle), pl.ds(middle, middle)):
        pairs.append((back.at[rows], back_to.at[rows]))
    pairs += [(gains, gains_to), (scales, scales_to)]
    for line in range(2 * lanes):
        unit, spot = divmod(line, lanes)
        gains[unit : unit + 1, 128 * spot : 128 * (spot + 1)] = lines[line : line + 1]
    scales[0] = lines[2 * lanes : 2 * lanes + 2]
    scales[1] = lines[2 * lanes + 2 : 2 * lanes + 4]
    copies = [
        pltpu.make_async_copy(source, target, sems.at[spot])
        for spot, (source, target) in enumerate(pairs)
    ]
    for made in copies:
        made.start()
    for made in copies:
        made.wait()


def wide_shape(rows, columns):
    steps = len(axis_bits("dp")) + len(axis_bits("seq"))
    return (2,) * steps + (rows >> steps, columns)


def sums_outputs(wide, lines):
    shapes = [
        jax.ShapeDtypeStruct((2, lax.axis_size("seq")) + shape[-2:], jnp.float32)
        for shape in wide[:2]
    ]
    return shapes + [jax.ShapeDtypeStruct(lines, jnp.float32)]


def reduced(partials, cuts, small, scaling):
    wide = [wide_shape(*partial.shape) for partial in partials]
    lines = small.reshape(-1, 128)
    space = pl.BlockSpec(memory_space=pltpu.VMEM)
    outs = sums_outputs(wide, lines.shape)
    made = pl.pallas_call(
        partial_of(gradient_kernel, cuts, scaling, len(partials)),
        out_shape=outs,
        in_specs=[space] * (len(partials) + 1),
        out_specs=[space] * len(outs),
        scratch_shapes=sums_scratch(cuts, wide, lines.shape),
        compiler_params=pltpu.CompilerParams(
            collective_id=0, has_side_effects=True, vmem_limit_bytes=24 << 20
        ),
        name="gradient_sums",
    )(*[value.reshape(shape) for value, shape in zip(partials, wide)], lines)
    sums = [value.reshape(2, -1, value.shape[-1]) for value in made[:2]]
    return sums, made[2].reshape(-1)


def whole_layer(frames, cotangent, weight_in, qk_scales, weight_out, gains, cuts, scaling):
    rows, model = frames.shape[0] * frames.shape[1], frames.shape[2]
    width, columns = weight_out.shape[1], weight_in.shape[2]
    shared = qk_scales.shape[-1]
    parts = rows // BLOCK
    blocked = (parts, 2, rows // CHUNK, CHUNK // (2 * parts), model)
    wide = [wide_shape(*pair) for pair in ((model, columns), (width, model)) * 2]
    wide[2], wide[3] = wide[3], wide[2]
    lines = (2 * model // 128 + 4 * shared // 128, 128)
    named = layer_scratch(rows, model, width, shared, parts)
    vmem, any_space = (
        pl.BlockSpec(memory_space=pltpu.VMEM),
        pl.BlockSpec(memory_space=pl.ANY),
    )
    outs = sums_outputs(wide, lines) + [
        jax.ShapeDtypeStruct(blocked, jnp.bfloat16),
        jax.ShapeDtypeStruct((rows, model), jnp.bfloat16),
    ]
    outs = [pltpu.VMEM(value.shape, value.dtype) for value in outs]
    made = pl.pallas_call(
        partial_of(layer_kernel, cuts, scaling, tuple(named)),
        out_shape=outs,
        in_specs=[any_space] * 6,
        out_specs=[vmem] * len(outs),
        scratch_shapes=list(named.values())
        + Unit.scratch(rows, model, width, shared) * 2
        + [pltpu.VMEM(shape, jnp.bfloat16) for shape in wide]
        + sums_scratch(cuts, wide, lines),
        compiler_params=pltpu.CompilerParams(
            collective_id=0, has_side_effects=True, vmem_limit_bytes=62 << 20
        ),
        name="layer_step",
    )(
        *[
            pltpu.with_memory_space_constraint(value, pltpu.HBM)
            for value in (
                frames.reshape(rows, model),
                cotangent.reshape(blocked),
                weight_in,
                weight_out,
                qk_scales,
                gains,
            )
        ]
    )
    handed = [made[3], made[4], made[0], made[1]]
    gin, gout, lines, out, back = made
    out, back, gin, gout, gain_sums, scale_sums = pl.pallas_call(
        handing_kernel,
        out_shape=[jax.ShapeDtypeStruct(value.shape, value.dtype) for value in handed]
        + [
            jax.ShapeDtypeStruct(gains.shape, jnp.float32),
            jax.ShapeDtypeStruct(qk_scales.shape, jnp.float32),
        ],
        in_specs=[vmem] * 5,
        out_specs=[any_space] * 6,
        scratch_shapes=[
            pltpu.VMEM(gains.shape, jnp.float32),
            pltpu.VMEM(qk_scales.shape, jnp.float32),
            pltpu.SemaphoreType.DMA((10,)),
        ],
        compiler_params=pltpu.CompilerParams(vmem_limit_bytes=4 << 20),
        name="handing",
    )(gin, gout, lines, out, back)
    sums = [value.reshape(2, -1, value.shape[-1]) for value in (gin, gout)]
    return out, back, *sums, gain_sums, scale_sums


def exchange(value, split, join):
    count = lax.axis_size("seq")
    me = lax.axis_index("seq")
    piece = value.shape[split] // count
    width = value.shape[join]
    shape = list(value.shape)
    shape[split] = piece
    shape[join] = width * count
    if count == 2:
        halves = jnp.split(value, 2, axis=split)
        own = jnp.where(me == 0, halves[0], halves[1])
        got = lax.ppermute(jnp.where(me == 0, halves[1], halves[0]), "seq", [(0, 1), (1, 0)])
        return jnp.concatenate(
            [jnp.where(me == 0, own, got), jnp.where(me == 0, got, own)], axis=join
        )
    out = jnp.zeros(shape, value.dtype)
    for step in range(count):
        other = jnp.bitwise_xor(me, step)
        part = lax.dynamic_slice_in_dim(value, other * piece, piece, split)
        if step:
            part = lax.ppermute(part, "seq", [(i, i ^ step) for i in range(count)])
        out = lax.dynamic_update_slice_in_dim(out, part, other * width, join)
    return out


def column_cuts(columns, parts):
    lanes = columns // 128
    ends = [128 * ((lanes * (i + 1)) // parts) for i in range(parts)]
    return list(zip([0] + ends[:-1], ends))


def column_cuts(columns, parts):
    grains = -(-columns // CHUNK)
    ends = [min(columns, CHUNK * ((grains * (i + 1)) // parts)) for i in range(parts)]
    return list(zip([0] + ends[:-1], ends))


CUTS = (
    (0, 0, 512, "yxzw"),
    (0, 512, 1024, "xzwy"),
    (0, 1024, 1536, "xyzw"),
    (0, 1536, 2176, "zxwy"),
    (1, 0, 256, "xzwy"),
    (1, 256, 512, "zyxw"),
    (2, 0, 256, "xzwy"),
    (2, 256, 512, "zyxw"),
    (3, 0, 384, "yxzw"),
    (3, 384, 768, "xywz"),
    (3, 768, 1152, "yxzw"),
    (3, 1152, 1536, "zxyw"),
    (3, 1536, 1920, "xzwy"),
    (3, 1920, 2176, "yxzw"),
)

HOOKS = {
    "h": (4,),
    "i0": (5,),
    "wb": (0, 1, 2, 3),
    "q0": (4, 5),
    "p1": (6, 1),
    "j0": (7,),
    "j2": (3,),
    "d0": (8,),
    "d1": (4, 9, 0, 2, 10, 11),
    "x": (12, 13, 5),
}

SECONDS_AT = ('j1', 'h')

LATE_FIRST = "P"
EARLY_OUT_FIRST = True

TAIL = (
    1, 6, 14, 7, 3, 8, 4, 9, 11, 2, 0, 1, 6, 10, 12, 2, 5, 14, 13, 0, 3, 8, 7, 11, 4, 12, 6, 10,
    9, 13, 2, 1, 14, 7, 5, 8, 3, 0, 11, 10, 6, 2, 12, 13, 14, 5, 9, 0, 7, 8, 11, 12, 10, 13, 9,
    14, 7, 8, 11, 10, 13, 9,
)


def plain_cuts(columns, model):
    cuts = []
    for array, (extent, parts) in enumerate(((columns, 3), (model, 2), (model, 2), (columns, 3))):
        for turn, (low, high) in enumerate(column_cuts(extent, parts)):
            cuts.append((array, low, high, turn + array))
    return cuts


def on_device(frames, cotangent, weight_in, qk_scales, weight_out, gains):
    block_count = frames.shape[1] // BLOCK
    width = frames.shape[2]
    ways = lax.axis_size("seq")
    tokens_all = frames.shape[0] * frames.shape[1] * lax.axis_size("dp") * ways
    scaling = tokens_all ** (-0.5)
    steps = len(axis_bits("dp")) + len(axis_bits("seq"))
    fits = (width >> steps) % 16 == 0 and ways == 2 and lax.axis_size("dp") == 16
    fits = fits and block_count == 2 and frames.shape[0] == 1
    fits = fits and weight_in.shape[2] == CUTS[-1][2]
    if fits:
        result, back_frames, *sums, gain_sums, scale_sums = whole_layer(
            frames, cotangent, weight_in, qk_scales, weight_out, gains, CUTS, scaling
        )
    else:
        blocked = frames.reshape(-1, BLOCK, width)
        upstream = exchange(cotangent.reshape(block_count, BLOCK, width), 1, 0)
        first, saved_first = unit_forward(
            blocked, weight_in[0], qk_scales[0], weight_out[0], gains[0], 1
        )
        first_pos = exchange(first, 1, 0)
        second, saved_second = unit_forward(
            first_pos, weight_in[1], qk_scales[1], weight_out[1], gains[1], 0
        )
        result = exchange(second, 0, 1)
        back_pos, *late = unit_backward(
            first_pos,
            upstream,
            weight_in[1],
            qk_scales[1],
            weight_out[1],
            gains[1],
            saved_second,
            0,
        )
        back_frames, *early = unit_backward(
            blocked,
            exchange(back_pos, 0, 1),
            weight_in[0],
            qk_scales[0],
            weight_out[0],
            gains[0],
            saved_first,
            1,
        )
        packed = jnp.concatenate(
            [early[2], late[2], early[3].reshape(-1), late[3].reshape(-1)]
        )
        grads = [value.astype(jnp.bfloat16) for value in (late[0], late[1], early[1], early[0])]
        cuts = plain_cuts(weight_in.shape[2], width)
        sums, small = reduced(grads, cuts, packed, scaling)
        gain_sums = small[: 2 * width].reshape(2, width)
        scale_sums = small[2 * width :].reshape(qk_scales.shape)
    return (
        result.reshape(frames.shape),
        back_frames.reshape(frames.shape),
        sums[0],
        sums[1],
        gain_sums,
        scale_sums,
    )


def solution(mesh):
    in_specs = (P("dp", "seq", None), P("dp", "seq", None), P(), P(), P(), P())
    out_specs = (
        P("dp", "seq", None),
        P("dp", "seq", None),
        P(None, "dp", None),
        P(None, "dp", None),
        P(),
        P(),
    )
    return jax.shard_map(
        on_device, mesh=mesh, in_specs=in_specs, out_specs=out_specs, check_vma=False
    )
```
